8 devices in a mesh: dp: 2 (over z, y), sp: 4 (over x, core).
Axes of the slice: x: 2, y: 2, z: 1, core: 2. Of those that a mesh axis runs over, the one named last changes fastest.
Arguments:
- images: bfloat16 [64, 32, 256, 32], P('dp', 'sp'), parts along dimension 0
- w_a: bfloat16 [2, 3, 3, 32, 32], replicated
- bn_a: float32 [2, 2, 32], replicated
- w_down: bfloat16 [3, 3, 32, 128], replicated
- bn_down: float32 [2, 128], replicated
- w_in: bfloat16 [3, 128, 64], replicated
- bn_in: float32 [3, 2, 64], replicated
- w_mid: bfloat16 [3, 3, 3, 64, 64], replicated
- bn_mid: float32 [3, 2, 64], replicated
- w_out: bfloat16 [3, 64, 128], replicated
- bn_out: float32 [3, 2, 128], replicated
Outputs:
- output: bfloat16 [64, 16, 128, 128], P('dp', 'sp'), parts along dimension 0
There are 2 independent parts. The reference program is written for one: setup_inputs(seed, part) draws one part's arguments, and reference() takes and returns one part's arrays. A program takes and returns all parts, laid end to end along the dimension named above; an argument that names none is the same for every part.
All inputs are finite; a program needn't handle non-finite values.
Results may differ from the reference program's by a relative error of at most 0.0191559.
Values are sent between devices in bfloat16 or wider.
A program may use at most 1 GiB of HBM per device.

```python
import jax
import jax.numpy as jnp
from jax import lax

IMAGES = 32
ROWS_DEV = 8
IMG_WIDTH = 256
LAYERS_A = 2
BLOCKS_B = 3
CHAN_A = 32
CHAN_MID = 64
CHAN_B = 128
GROUP_SIZE = 4
NORM_EPS = 1e-5
CONV_DIMS = ("NHWC", "HWIO", "NHWC")


def conv_weight(draw_key, full_shape, fan_in):
    return (jax.random.normal(draw_key, full_shape, jnp.float32) * fan_in ** -0.5).astype(jnp.bfloat16)


def norm_params(draw_key, lead_dims, chan_count):
    key_gain, key_shift = jax.random.split(draw_key)
    norm_gain = jax.random.uniform(key_gain, lead_dims + (chan_count,), jnp.float32, 0.6, 1.4)
    norm_shift = 0.4 * jax.random.normal(key_shift, lead_dims + (chan_count,), jnp.float32)
    return jnp.stack([norm_gain, norm_shift], axis=-2)


def setup_inputs(seed: int = 0, part: int = 0) -> dict:
    base_key = jax.random.key(seed)
    part_key = jax.random.fold_in(base_key, part)
    key_noise, key_amp, key_phase = jax.random.split(part_key, 3)
    weight_keys = jax.random.split(base_key, 10)
    height = GROUP_SIZE * ROWS_DEV
    row_pos = (jnp.arange(height, dtype=jnp.float32) + 0.5) / height
    band_amp = 1.5 * jax.random.normal(key_amp, (CHAN_A,), jnp.float32)
    band_phase = 6.2832 * jax.random.uniform(key_phase, (CHAN_A,), jnp.float32)
    row_band = band_amp * (1.0 - 2.0 * row_pos)[:, None] + jnp.sin(12.566 * row_pos[:, None] + band_phase)
    pixel_noise = jax.random.normal(key_noise, (IMAGES, height, IMG_WIDTH, CHAN_A), jnp.float32)
    return {
        "images": (pixel_noise + row_band[None, :, None, :]).astype(jnp.bfloat16),
        "w_a": conv_weight(weight_keys[0], (LAYERS_A, 3, 3, CHAN_A, CHAN_A), 9 * CHAN_A),
        "bn_a": norm_params(weight_keys[1], (LAYERS_A,), CHAN_A),
        "w_down": conv_weight(weight_keys[2], (3, 3, CHAN_A, CHAN_B), 9 * CHAN_A),
        "bn_down": norm_params(weight_keys[3], (), CHAN_B),
        "w_in": conv_weight(weight_keys[4], (BLOCKS_B, CHAN_B, CHAN_MID), CHAN_B),
        "bn_in": norm_params(weight_keys[5], (BLOCKS_B,), CHAN_MID),
        "w_mid": conv_weight(weight_keys[6], (BLOCKS_B, 3, 3, CHAN_MID, CHAN_MID), 9 * CHAN_MID),
        "bn_mid": norm_params(weight_keys[7], (BLOCKS_B,), CHAN_MID),
        "w_out": conv_weight(weight_keys[8], (BLOCKS_B, CHAN_MID, CHAN_B), CHAN_MID),
        "bn_out": norm_params(weight_keys[9], (BLOCKS_B,), CHAN_B),
    }


def conv_full(hidden, weight, stride):
    return lax.conv_general_dilated(hidden.astype(jnp.float32), weight.astype(jnp.float32), (stride, stride), "SAME", dimension_numbers=CONV_DIMS)


def conv_point(hidden, weight):
    return jnp.einsum("bhwc,cd->bhwd", hidden.astype(jnp.float32), weight.astype(jnp.float32))


def batch_norm(pre_act, params):
    chan_mean = jnp.mean(pre_act, axis=(0, 1, 2))
    chan_var = jnp.mean(pre_act * pre_act, axis=(0, 1, 2)) - chan_mean * chan_mean
    chan_scale = params[0] * lax.rsqrt(chan_var + NORM_EPS)
    return (pre_act - chan_mean) * chan_scale + params[1]


def norm_relu(pre_act, params):
    return jax.nn.relu(batch_norm(pre_act, params)).astype(jnp.bfloat16)


def reference(images, w_a, bn_a, w_down, bn_down, w_in, bn_in, w_mid, bn_mid, w_out, bn_out):
    def stage_a(hidden, layer_args):
        return norm_relu(conv_full(hidden, layer_args[0], 1), layer_args[1]), None

    def bottleneck(hidden, block_args):
        w_first, bn_first, w_three, bn_three, w_last, bn_last = block_args
        branch = norm_relu(conv_point(hidden, w_first), bn_first)
        branch = norm_relu(conv_full(branch, w_three, 1), bn_three)
        summed = batch_norm(conv_point(branch, w_last), bn_last) + hidden.astype(jnp.float32)
        return jax.nn.relu(summed).astype(jnp.bfloat16), None

    hidden, _ = lax.scan(stage_a, images, (w_a, bn_a))
    hidden = norm_relu(conv_full(hidden, w_down, 2), bn_down)
    hidden, _ = lax.scan(bottleneck, hidden, (w_in, bn_in, w_mid, bn_mid, w_out, bn_out))
    return hidden
```

```python
import jax
import jax.numpy as jnp
from jax import lax
from jax.experimental import pallas as pl
from jax.experimental.pallas import tpu as pltpu
from jax.sharding import PartitionSpec as P

NORM_EPS = 1e-5
MESH = pl.DeviceIdType.MESH
F32 = jnp.float32
BF16 = jnp.bfloat16
ROWS_A = 8
ROWS_B = 4
LANES = 256


def band(weight, taps_h, taps_w, phases):
    kernel = jnp.transpose(weight, (3, 0, 1, 2))
    free_h, free_w = taps_h - 3, taps_w - 3
    blocks = []
    for row in range(free_h + 1):
        for phase in phases:
            blocks.append(jnp.pad(kernel, ((0, 0), (row, free_h - row), (phase, free_w - phase), (0, 0))))
    out = jnp.concatenate(blocks, axis=0)
    return out.reshape(out.shape[0], taps_h * taps_w * weight.shape[2])


def solution(mesh):
    groups = mesh.shape["sp"]

    def kernel(x_hbm, wa, wd, wi, wm, wo, bn, out_hbm,
               xv, xh, hs, us, za, zb, hb, ov, acc, ab, stat,
               x_sem, out_sem, halo_send, halo_recv, stat_send, stat_recv):
        pairs = xv.shape[0]
        me = lax.axis_index("sp")
        count_a = float(2 * pairs * ROWS_A * LANES * groups)
        count_b = float(2 * pairs * ROWS_B * 128 * groups)

        def x_copy(pair):
            return pltpu.make_async_copy(x_hbm.at[pl.ds(2 * pair, 2)], xv.at[pair], x_sem.at[pair])

        @pl.loop(0, pairs)
        def _(pair):
            x_copy(pair).start()

        barrier = pltpu.get_barrier_semaphore()
        for hop in range(1, groups):
            pl.semaphore_signal(barrier, inc=1, device_id={"sp": lax.rem(me + hop, groups)}, device_id_type=MESH)
        pl.semaphore_wait(barrier, groups - 1)

        def halo_copy(step, side, src, dst):
            peer = me + 1 if side == 0 else me - 1
            return pltpu.make_async_remote_copy(
                src_ref=src, dst_ref=dst, send_sem=halo_send.at[step, side], recv_sem=halo_recv.at[step, side],
                device_id={"sp": peer}, device_id_type=MESH)

        def has_peer(side):
            return me < groups - 1 if side == 0 else me > 0

        def from_peer(side):
            return me > 0 if side == 0 else me < groups - 1

        def exchange(step, side, src, dst):
            @pl.when(has_peer(side))
            def _():
                halo_copy(step, side, src, dst).start()

        def settle(step, side, src, dst):
            @pl.when(from_peer(side))
            def _():
                pltpu.make_async_remote_copy(
                    src_ref=src, dst_ref=dst, send_sem=halo_send.at[step, side], recv_sem=halo_recv.at[step, side],
                    device_id={"sp": me}, device_id_type=MESH).wait_recv()

            @pl.when(has_peer(side))
            def _():
                halo_copy(step, side, src, dst).wait_send()

        x_src = (x_hbm.at[:, ROWS_A - 1], x_hbm.at[:, 0])
        x_dst = (xh.at[0], xh.at[1])
        for side in range(2):
            exchange(0, side, x_src[side], x_dst[side])

        @pl.when(me == 0)
        def _():
            xh[0] = jnp.zeros(xh.shape[1:], BF16)

            @pl.loop(0, pairs)
            def _(pair):
                hs[pair, 0] = jnp.zeros(hs.shape[2:], BF16)
                us[pair, 0] = jnp.zeros(us.shape[2:], BF16)

        @pl.when(me == groups - 1)
        def _():
            xh[1] = jnp.zeros(xh.shape[1:], BF16)

            @pl.loop(0, pairs)
            def _(pair):
                hs[pair, ROWS_A + 1] = jnp.zeros(hs.shape[2:], BF16)
                us[pair, ROWS_B + 1] = jnp.zeros(us.shape[2:], BF16)

        def shift(value, step):
            lane = lax.broadcasted_iota(jnp.int32, (value.shape[0], 128), 1)
            edge = 0 if step == 1 else 127
            halves = []
            for half in range(2):
                moved = pltpu.roll(value[:, half * 128:(half + 1) * 128], step % 128, 1)
                halves.append(jnp.where(lane == edge, 0.0, moved))
            return jnp.concatenate(halves, axis=1)

        def put_planes(pair, row, even, odd, centre=True):
            hs[pair, row, 0:32] = shift(odd, 1).astype(BF16)
            if centre:
                hs[pair, row, 32:64] = even.astype(BF16)
                hs[pair, row, 64:96] = odd.astype(BF16)
            hs[pair, row, 96:128] = shift(even, -1).astype(BF16)

        def put_mid(pair, row, value, centre=True):
            us[pair, row, 0:64] = shift(value, 1).astype(BF16)
            if centre:
                us[pair, row, 64:128] = value.astype(BF16)
            us[pair, row, 128:192] = shift(value, -1).astype(BF16)

        def rebuild_a(pair, row):
            both = hs[pair, row, 32:96].astype(F32)
            put_planes(pair, row, both[0:32], both[32:64], centre=False)

        def rebuild_mid(pair, row):
            put_mid(pair, row, us[pair, row, 64:128].astype(F32), centre=False)

        def clear():
            acc[...] = jnp.zeros(acc.shape, F32)

        def tally(value):
            left, right = value[:, :128], value[:, 128:]
            rows = value.shape[0]
            acc[0, 0:rows] += left + right
            acc[1, 0:rows] += left * left + right * right

        def moments(layer, channels, count):
            for part in range(2):
                turned = acc[part].T.reshape(16, 8, 128)
                stat[layer, me, 8 * part:8 * part + 8] = jnp.sum(turned, axis=0)
            copies = []
            for hop in range(1, groups):
                copies.append(pltpu.make_async_remote_copy(
                    src_ref=stat.at[layer, me], dst_ref=stat.at[layer, me],
                    send_sem=stat_send.at[layer, hop], recv_sem=stat_recv.at[layer, hop],
                    device_id={"sp": lax.rem(me + hop, groups)}, device_id_type=MESH))
            for copy in copies:
                copy.start()
            for hop in range(1, groups):
                origin = lax.rem(me + groups - hop, groups)
                pltpu.make_async_remote_copy(
                    src_ref=stat.at[layer, origin], dst_ref=stat.at[layer, origin],
                    send_sem=stat_send.at[layer, hop], recv_sem=stat_recv.at[layer, hop],
                    device_id={"sp": origin}, device_id_type=MESH).wait_recv()
            for copy in copies:
                copy.wait_send()
            total = stat[layer, 0]
            for origin in range(1, groups):
                total = total + stat[layer, origin]

            def fold(block):
                line = jnp.broadcast_to(jnp.sum(block, axis=0, keepdims=True), (8, 128))
                width = 64
                while width >= channels:
                    line = line + pltpu.roll(line, width, 1)
                    width //= 2
                return line / count

            mean, square = fold(total[0:8]), fold(total[8:16])
            var = square - mean * mean
            scale = bn[layer, 0:1] * lax.rsqrt(var + NORM_EPS)
            bias = bn[layer, 1:2] - mean * scale
            ab[0] = jnp.broadcast_to(scale[0:1], (128, 128)).T
            ab[1] = jnp.broadcast_to(bias[0:1], (128, 128)).T
            clear()

        def affine(value):
            rows = value.shape[0]
            scale, bias = ab[0, 0:rows], ab[1, 0:rows]
            return jnp.concatenate(
                [value[:, :128] * scale + bias, value[:, 128:] * scale + bias], axis=1)

        def norm_relu(value):
            return jnp.maximum(affine(value), 0.0)

        def mm(left, right):
            return jnp.dot(left, right, preferred_element_type=F32)

        clear()

        lane_in = lax.broadcasted_iota(jnp.int32, (LANES, LANES), 0)
        lane_out = lax.broadcasted_iota(jnp.int32, (LANES, LANES), 1)
        source = jnp.where(lane_out < 128, 2 * lane_out, 2 * lane_out - (LANES - 1))
        perm = jnp.where(lane_in == source, 1.0, 0.0).astype(BF16)

        def split_rows(first, second, pair, row):
            one, two = mm(first, perm), mm(second, perm)
            put_planes(pair, row, jnp.concatenate([one[:, :128], two[:, :128]], axis=1),
                       jnp.concatenate([one[:, 128:], two[:, 128:]], axis=1))

        def conv_a(layer, pair, row, rows):
            window = hs[pair, row:row + rows + 2].reshape((rows + 2) * 128, LANES)
            value = mm(wa[layer, 0:64 * rows, 0:128 * (rows + 2)], window)
            tally(value)
            za[pl.ds(pair * ROWS_A + row, rows)] = value.reshape(rows, 64, LANES)

        def norm_a(pair, row):
            value = norm_relu(za[pair * ROWS_A + row])
            put_planes(pair, row + 1, value[0:32], value[32:64])

        @pl.loop(0, pairs)
        def _(pair):
            x_copy(pair).wait()
            for row in range(ROWS_A):
                split_rows(xv[pair, 0, row], xv[pair, 1, row], pair, row + 1)
            for row in range(1, ROWS_A - 1, 2):
                conv_a(0, pair, row, 2)

        for side in range(2):
            settle(0, side, x_src[side], x_dst[side])

        @pl.loop(0, pairs)
        def _(pair):
            split_rows(xh[0, 2 * pair], xh[0, 2 * pair + 1], pair, 0)
            split_rows(xh[1, 2 * pair], xh[1, 2 * pair + 1], pair, ROWS_A + 1)
            conv_a(0, pair, 0, 1)
            conv_a(0, pair, ROWS_A - 1, 1)

        moments(0, 32, count_a)

        a_src = (hs.at[:, ROWS_A, 32:96], hs.at[:, 1, 32:96])
        a_dst = (hs.at[:, 0, 32:96], hs.at[:, ROWS_A + 1, 32:96])

        @pl.loop(0, pairs)
        def _(pair):
            norm_a(pair, 0)
            norm_a(pair, ROWS_A - 1)

        for side in range(2):
            exchange(1, side, a_src[side], a_dst[side])

        @pl.loop(0, pairs)
        def _(pair):
            for row in range(1, ROWS_A - 1):
                norm_a(pair, row)
            for row in range(1, ROWS_A - 1, 2):
                conv_a(1, pair, row, 2)

        for side in range(2):
            settle(1, side, a_src[side], a_dst[side])

        @pl.loop(0, pairs)
        def _(pair):
            rebuild_a(pair, 0)
            rebuild_a(pair, ROWS_A + 1)
            conv_a(1, pair, 0, 1)
            conv_a(1, pair, ROWS_A - 1, 1)

        moments(1, 32, count_a)

        def conv_down(pair, row):
            window = hs[pair, 2 * row + 1:2 * row + 4].reshape(384, LANES)
            value = mm(wd[...], window)
            tally(value)
            zb[pair * ROWS_B + row] = value

        @pl.loop(0, pairs)
        def _(pair):
            norm_a(pair, 0)

        exchange(2, 1, a_src[1], a_dst[1])

        @pl.loop(0, pairs)
        def _(pair):
            for row in range(1, ROWS_A):
                norm_a(pair, row)
            for row in range(ROWS_B - 1):
                conv_down(pair, row)

        settle(2, 1, a_src[1], a_dst[1])

        @pl.loop(0, pairs)
        def _(pair):
            rebuild_a(pair, ROWS_A + 1)
            conv_down(pair, ROWS_B - 1)

        moments(2, 128, count_b)

        def conv_in(block, index, hidden):
            value = mm(wi[block], hidden)
            tally(value)
            za[index] = value

        def conv_mid(block, pair, row, rows):
            window = us[pair, row:row + rows + 2].reshape((rows + 2) * 192, LANES)
            value = mm(wm[block, 0:64 * rows, 0:192 * (rows + 2)], window)
            tally(value)
            za[pl.ds(pair * ROWS_B + row, rows)] = value.reshape(rows, 64, LANES)

        def norm_mid(pair, row):
            put_mid(pair, row + 1, norm_relu(za[pair * ROWS_B + row]))

        m_src = (us.at[:, ROWS_B, 64:128], us.at[:, 1, 64:128])
        m_dst = (us.at[:, 0, 64:128], us.at[:, ROWS_B + 1, 64:128])

        @pl.loop(0, pairs)
        def _(pair):
            for row in range(ROWS_B):
                index = pair * ROWS_B + row
                hidden = norm_relu(zb[index]).astype(BF16)
                hb[index] = hidden
                conv_in(0, index, hidden)

        blocks = wi.shape[0]
        for block in range(blocks):
            layer, step = 3 + 3 * block, 3 + block
            moments(layer, 64, count_b)

            @pl.loop(0, pairs)
            def _(pair):
                norm_mid(pair, 0)
                norm_mid(pair, ROWS_B - 1)

            for side in range(2):
                exchange(step, side, m_src[side], m_dst[side])

            @pl.loop(0, pairs)
            def _(pair):
                for row in range(1, ROWS_B - 1):
                    norm_mid(pair, row)
                conv_mid(block, pair, 1, 2)

            for side in range(2):
                settle(step, side, m_src[side], m_dst[side])

            @pl.loop(0, pairs)
            def _(pair):
                rebuild_mid(pair, 0)
                rebuild_mid(pair, ROWS_B + 1)
                conv_mid(block, pair, 0, 1)
                conv_mid(block, pair, ROWS_B - 1, 1)

            moments(layer + 1, 64, count_b)

            @pl.loop(0, pairs)
            def _(pair):
                for row in range(ROWS_B):
                    index = pair * ROWS_B + row
                    value = mm(wo[block], norm_relu(za[index]).astype(BF16))
                    tally(value)
                    zb[index] = value

            moments(layer + 2, 128, count_b)

            def finish(index):
                return jnp.maximum(affine(zb[index]) + hb[index].astype(F32), 0.0)

            if block < blocks - 1:
                @pl.loop(0, pairs)
                def _(pair):
                    for row in range(ROWS_B):
                        index = pair * ROWS_B + row
                        hidden = finish(index).astype(BF16)
                        hb[index] = hidden
                        conv_in(block + 1, index, hidden)
            else:
                def out_copy(pair):
                    return pltpu.make_async_copy(ov.at[pair], out_hbm.at[pl.ds(2 * pair, 2)], out_sem.at[pair])

                @pl.loop(0, pairs)
                def _(pair):
                    for row in range(ROWS_B):
                        value = finish(pair * ROWS_B + row)
                        for image in range(2):
                            ov[pair, image, row] = value[:, image * 128:(image + 1) * 128].T.astype(BF16)
                    out_copy(pair).start()

                @pl.loop(0, pairs)
                def _(pair):
                    out_copy(pair).wait()

    def forward(images, w_a, bn_a, w_down, bn_down, w_in, bn_in, w_mid, bn_mid, w_out, bn_out):
        images_count = images.shape[0]
        pairs = images_count // 2
        x = jnp.transpose(images, (0, 1, 3, 2))
        wa = jnp.stack([band(w_a[layer], 4, 4, (0, 1)) for layer in range(w_a.shape[0])])
        wd = band(w_down, 3, 4, (1,))
        wi = jnp.transpose(w_in, (0, 2, 1))
        wm = jnp.stack([band(w_mid[block], 4, 3, (0,)) for block in range(w_mid.shape[0])])
        wo = jnp.transpose(w_out, (0, 2, 1))
        bn = [jnp.tile(bn_a[layer], (1, 4)) for layer in range(w_a.shape[0])] + [bn_down]
        for block in range(w_in.shape[0]):
            bn += [jnp.tile(bn_in[block], (1, 2)), jnp.tile(bn_mid[block], (1, 2)), bn_out[block]]
        bn = jnp.stack(bn)
        layers = bn.shape[0]
        steps = 3 + w_in.shape[0]
        vmem = pl.BlockSpec(memory_space=pltpu.VMEM)
        hbm = pl.BlockSpec(memory_space=pl.ANY)
        dma = pltpu.SemaphoreType.DMA
        return pl.pallas_call(
            kernel,
            out_shape=jax.ShapeDtypeStruct((images_count, ROWS_B, 128, 128), BF16),
            in_specs=[hbm] + [vmem] * 6,
            out_specs=hbm,
            scratch_shapes=[
                pltpu.VMEM((pairs, 2, ROWS_A, 32, LANES), BF16),
                pltpu.VMEM((2, images_count, 32, LANES), BF16),
                pltpu.VMEM((pairs, ROWS_A + 2, 128, LANES), BF16),
                pltpu.VMEM((pairs, ROWS_B + 2, 192, LANES), BF16),
                pltpu.VMEM((pairs * ROWS_A, 64, LANES), F32),
                pltpu.VMEM((pairs * ROWS_B, 128, LANES), F32),
                pltpu.VMEM((pairs * ROWS_B, 128, LANES), BF16),
                pltpu.VMEM((pairs, 2, ROWS_B, 128, 128), BF16),
                pltpu.VMEM((2, 128, 128), F32),
                pltpu.VMEM((2, 128, 128), F32),
                pltpu.VMEM((layers, groups, 16, 128), F32),
                dma((pairs,)), dma((pairs,)), dma((steps, 2)), dma((steps, 2)),
                dma((layers, groups)), dma((layers, groups)),
            ],
            compiler_params=pltpu.CompilerParams(
                collective_id=0, has_side_effects=True, vmem_limit_bytes=67043328),
            name="conv_stack",
        )(x, wa, wd, wi, wm, wo, bn)

    act_spec = P("dp", "sp", None, None)
    return jax.shard_map(forward, mesh=mesh, in_specs=(act_spec,) + (P(),) * 10, out_specs=act_spec, check_vma=False)
```

```python
import jax
import jax.numpy as jnp
from jax import lax
from jax.experimental import pallas as pl
from jax.experimental.pallas import tpu as pltpu
from jax.sharding import PartitionSpec as P

NORM_EPS = 1e-5
MESH = pl.DeviceIdType.MESH
F32 = jnp.float32
BF16 = jnp.bfloat16
ROWS_A = 8
ROWS_B = 4
UNROLL = 4
LANES = 256


def solution(mesh):
    groups = mesh.shape["sp"]

    def kernel(x_hbm, raw_a, bn_a, raw_d, bn_d, wi, bn_i, raw_m, bn_m, raw_o, bn_o, out_hbm,
               wa, wd, wm, wo, xv, xh, hs, us, za, zb, hb, ov, acc, ab, stat,
               x_sem, out_sem, halo_send, halo_recv, stat_send, stat_recv):
        pairs = xv.shape[0]
        me = lax.axis_index("sp")
        count_a = float(2 * pairs * ROWS_A * LANES * groups)
        count_b = float(2 * pairs * ROWS_B * 128 * groups)

        def sweep(body, unroll=UNROLL):
            @pl.loop(0, pairs // unroll)
            def _(step):
                sums = [body(step * unroll + part) for part in range(unroll)]
                if sums[0] is not None:
                    channels = sums[0].shape[1]
                    acc[:, 0:channels] += sum(sums[1:], sums[0])

        def x_copy(pair):
            return pltpu.make_async_copy(x_hbm.at[pl.ds(2 * pair, 2)], xv.at[pair], x_sem.at[pair])

        @sweep
        def _(pair):
            x_copy(pair).start()

        barrier = pltpu.get_barrier_semaphore()
        for hop in range(1, groups):
            pl.semaphore_signal(barrier, inc=1, device_id={"sp": lax.rem(me + hop, groups)}, device_id_type=MESH)
        pl.semaphore_wait(barrier, groups - 1)

        def halo_copy(step, side, src, dst):
            peer = me + 1 if side == 0 else me - 1
            return pltpu.make_async_remote_copy(
                src_ref=src, dst_ref=dst, send_sem=halo_send.at[step, side], recv_sem=halo_recv.at[step, side],
                device_id={"sp": peer}, device_id_type=MESH)

        def has_peer(side):
            return me < groups - 1 if side == 0 else me > 0

        def from_peer(side):
            return me > 0 if side == 0 else me < groups - 1

        def exchange(step, side, src, dst):
            @pl.when(has_peer(side))
            def _():
                halo_copy(step, side, src, dst).start()

        def settle(step, side, src, dst):
            @pl.when(from_peer(side))
            def _():
                pltpu.make_async_remote_copy(
                    src_ref=src, dst_ref=dst, send_sem=halo_send.at[step, side], recv_sem=halo_recv.at[step, side],
                    device_id={"sp": me}, device_id_type=MESH).wait_recv()

            @pl.when(has_peer(side))
            def _():
                halo_copy(step, side, src, dst).wait_send()

        x_src = (x_hbm.at[:, ROWS_A - 1], x_hbm.at[:, 0])
        x_dst = (xh.at[0], xh.at[1])
        for side in range(2):
            exchange(0, side, x_src[side], x_dst[side])

        @pl.when(me == 0)
        def _():
            xh[0] = jnp.zeros(xh.shape[1:], BF16)

            @sweep
            def _(pair):
                hs[pair, 0] = jnp.zeros(hs.shape[2:], BF16)
                us[pair, 0] = jnp.zeros(us.shape[2:], BF16)

        @pl.when(me == groups - 1)
        def _():
            xh[1] = jnp.zeros(xh.shape[1:], BF16)

            @sweep
            def _(pair):
                hs[pair, ROWS_A + 1] = jnp.zeros(hs.shape[2:], BF16)
                us[pair, ROWS_B + 1] = jnp.zeros(us.shape[2:], BF16)

        def turn(block):
            return block.astype(F32).T.astype(BF16)

        def prepare_a(layer):
            for row in range(4):
                lines = []
                for plane in range(4):
                    tiles = []
                    for out_row in range(2):
                        for phase in range(2):
                            high, wide = row - out_row, plane - phase
                            inside = 0 <= high < 3 and 0 <= wide < 3
                            tiles.append(raw_a[layer, high, wide].astype(F32) if inside else jnp.zeros((32, 32), F32))
                    lines.append(jnp.concatenate(tiles, axis=1))
                wa[layer, :, 128 * row:128 * row + 128] = turn(jnp.concatenate(lines, axis=0))

        def prepare_down():
            for high in range(3):
                lines = [jnp.zeros((32, 128), BF16)] + [raw_d[high, wide] for wide in range(3)]
                wd[:, 128 * high:128 * high + 128] = turn(jnp.concatenate(lines, axis=0))

        def prepare_block(block):
            lines = []
            for row in range(4):
                for wide in range(3):
                    tiles = []
                    for out_row in range(2):
                        high = row - out_row
                        inside = 0 <= high < 3
                        tiles.append(raw_m[block, high, wide].astype(F32) if inside else jnp.zeros((64, 64), F32))
                    lines.append(jnp.concatenate(tiles, axis=1))
            for part in range(6):
                wm[block, :, 128 * part:128 * part + 128] = turn(jnp.concatenate(lines[2 * part:2 * part + 2], axis=0))
            wo[block] = turn(raw_o[block])

        def shift(value, step):
            lane = lax.broadcasted_iota(jnp.int32, (value.shape[0], 128), 1)
            edge = 0 if step == 1 else 127
            halves = []
            for half in range(2):
                moved = pltpu.roll(value[:, half * 128:(half + 1) * 128], step % 128, 1)
                halves.append(jnp.where(lane == edge, 0.0, moved))
            return jnp.concatenate(halves, axis=1)

        def put_planes(pair, row, even, odd, centre=True):
            hs[pair, row, 0:32] = shift(odd, 1).astype(BF16)
            if centre:
                hs[pair, row, 32:64] = even.astype(BF16)
                hs[pair, row, 64:96] = odd.astype(BF16)
            hs[pair, row, 96:128] = shift(even, -1).astype(BF16)

        def put_mid(pair, row, value, centre=True):
            us[pair, row, 0:64] = shift(value, 1).astype(BF16)
            if centre:
                us[pair, row, 64:128] = value.astype(BF16)
            us[pair, row, 128:192] = shift(value, -1).astype(BF16)

        def rebuild_a(pair, row):
            both = hs[pair, row, 32:96].astype(F32)
            put_planes(pair, row, both[0:32], both[32:64], centre=False)

        def rebuild_mid(pair, row):
            put_mid(pair, row, us[pair, row, 64:128].astype(F32), centre=False)

        def clear():
            acc[...] = jnp.zeros(acc.shape, F32)

        def tally(channels, *values):
            total, square = 0.0, 0.0
            for value in values:
                for half in range(2):
                    for row in range(0, value.shape[0], channels):
                        piece = value[row:row + channels, half * 128:(half + 1) * 128]
                        total, square = total + piece, square + piece * piece
            return jnp.stack([total, square])

        def moments(layer, params, count, during=None):
            channels = params.shape[1]
            for part in range(2):
                turned = acc[part].T.reshape(16, 8, 128)
                stat[layer, me, 8 * part:8 * part + 8] = jnp.sum(turned, axis=0)
            copies = []
            for hop in range(1, groups):
                copies.append(pltpu.make_async_remote_copy(
                    src_ref=stat.at[layer, me], dst_ref=stat.at[layer, me],
                    send_sem=stat_send.at[layer, hop], recv_sem=stat_recv.at[layer, hop],
                    device_id={"sp": lax.rem(me + hop, groups)}, device_id_type=MESH))
            for copy in copies:
                copy.start()
            clear()
            if during is not None:
                during()
            for hop in range(1, groups):
                origin = lax.rem(me + groups - hop, groups)
                pltpu.make_async_remote_copy(
                    src_ref=stat.at[layer, origin], dst_ref=stat.at[layer, origin],
                    send_sem=stat_send.at[layer, hop], recv_sem=stat_recv.at[layer, hop],
                    device_id={"sp": origin}, device_id_type=MESH).wait_recv()
            for copy in copies:
                copy.wait_send()
            total = stat[layer, 0]
            for origin in range(1, groups):
                total = total + stat[layer, origin]

            def fold(block):
                line = jnp.broadcast_to(jnp.sum(block, axis=0, keepdims=True), (8, 128))
                width = 64
                while width >= channels:
                    line = line + pltpu.roll(line, width, 1)
                    width //= 2
                return line / count

            mean, square = fold(total[0:8]), fold(total[8:16])
            var = square - mean * mean
            wide = jnp.concatenate([params] * (128 // channels), axis=1)
            scale = wide[0:1] * lax.rsqrt(var + NORM_EPS)
            bias = wide[1:2] - mean * scale
            ab[0] = jnp.broadcast_to(scale[0:1], (128, 128)).T
            ab[1] = jnp.broadcast_to(bias[0:1], (128, 128)).T

        def affine(value):
            rows = value.shape[0]
            scale, bias = ab[0, 0:rows], ab[1, 0:rows]
            return jnp.concatenate(
                [value[:, :128] * scale + bias, value[:, 128:] * scale + bias], axis=1)

        def norm_relu(value):
            return jnp.maximum(affine(value), 0.0)

        def mm(left, right):
            return jnp.dot(left, right, preferred_element_type=F32)

        clear()
        for layer in range(wa.shape[0]):
            prepare_a(layer)

        lane_in = lax.broadcasted_iota(jnp.int32, (LANES, LANES), 0)
        lane_out = lax.broadcasted_iota(jnp.int32, (LANES, LANES), 1)
        source = jnp.where(lane_out < 128, 2 * lane_out, 2 * lane_out - (LANES - 1))
        perm = jnp.where(lane_in == source, 1.0, 0.0).astype(BF16)

        def split_rows(first, second, pair, row):
            put_planes(pair, row, jnp.concatenate([first[:, :128], second[:, :128]], axis=1),
                       jnp.concatenate([first[:, 128:], second[:, 128:]], axis=1))

        def conv_a(layer, pair, row, rows):
            window = hs[pair, row:row + rows + 2].reshape((rows + 2) * 128, LANES)
            value = mm(wa[layer, 0:64 * rows, 0:128 * (rows + 2)], window)
            za[pl.ds(pair * ROWS_A + row, rows)] = value.reshape(rows, 64, LANES)
            return value

        def norm_a(pair, row):
            value = norm_relu(za[pair * ROWS_A + row])
            put_planes(pair, row + 1, value[0:32], value[32:64])

        @sweep
        def _(pair):
            x_copy(pair).wait()
            both = mm(xv[pair].reshape(2 * ROWS_A * 32, LANES), perm).reshape(2, ROWS_A, 32, LANES)
            for row in range(ROWS_A):
                split_rows(both[0, row], both[1, row], pair, row + 1)
            return tally(32, *[conv_a(0, pair, row, 2) for row in range(1, ROWS_A - 1, 2)])

        for side in range(2):
            settle(0, side, x_src[side], x_dst[side])

        @sweep
        def _(pair):
            both = mm(xh[:, pl.ds(2 * pair, 2)].reshape(4 * 32, LANES), perm).reshape(2, 2, 32, LANES)
            split_rows(both[0, 0], both[0, 1], pair, 0)
            split_rows(both[1, 0], both[1, 1], pair, ROWS_A + 1)
            return tally(32, conv_a(0, pair, 0, 1), conv_a(0, pair, ROWS_A - 1, 1))

        moments(0, bn_a[0], count_a, prepare_down)

        a_src = (hs.at[:, ROWS_A, 32:96], hs.at[:, 1, 32:96])
        a_dst = (hs.at[:, 0, 32:96], hs.at[:, ROWS_A + 1, 32:96])

        @sweep
        def _(pair):
            norm_a(pair, 0)
            norm_a(pair, ROWS_A - 1)

        for side in range(2):
            exchange(1, side, a_src[side], a_dst[side])

        @sweep
        def _(pair):
            for row in range(1, ROWS_A - 1):
                norm_a(pair, row)
            return tally(32, *[conv_a(1, pair, row, 2) for row in range(1, ROWS_A - 1, 2)])

        for side in range(2):
            settle(1, side, a_src[side], a_dst[side])

        @sweep
        def _(pair):
            rebuild_a(pair, 0)
            rebuild_a(pair, ROWS_A + 1)
            return tally(32, conv_a(1, pair, 0, 1), conv_a(1, pair, ROWS_A - 1, 1))

        moments(1, bn_a[1], count_a, lambda: prepare_block(0))

        def conv_down(pair, row):
            window = hs[pair, 2 * row + 1:2 * row + 4].reshape(384, LANES)
            value = mm(wd[...], window)
            zb[pair * ROWS_B + row] = value
            return value

        @sweep
        def _(pair):
            norm_a(pair, 0)

        exchange(2, 1, a_src[1], a_dst[1])

        @sweep
        def _(pair):
            for row in range(1, ROWS_A):
                norm_a(pair, row)
            return tally(128, *[conv_down(pair, row) for row in range(ROWS_B - 1)])

        settle(2, 1, a_src[1], a_dst[1])

        @sweep
        def _(pair):
            rebuild_a(pair, ROWS_A + 1)
            return tally(128, conv_down(pair, ROWS_B - 1))

        moments(2, bn_d[...], count_b, lambda: prepare_block(1))

        def conv_in(block, index, hidden):
            value = mm(wi[block], hidden)
            za[index] = value
            return value

        def conv_mid(block, pair, row, rows):
            window = us[pair, row:row + rows + 2].reshape((rows + 2) * 192, LANES)
            value = mm(wm[block, 0:64 * rows, 0:192 * (rows + 2)], window)
            za[pl.ds(pair * ROWS_B + row, rows)] = value.reshape(rows, 64, LANES)
            return value

        def norm_mid(pair, row):
            put_mid(pair, row + 1, norm_relu(za[pair * ROWS_B + row]))

        m_src = (us.at[:, ROWS_B, 64:128], us.at[:, 1, 64:128])
        m_dst = (us.at[:, 0, 64:128], us.at[:, ROWS_B + 1, 64:128])

        @sweep
        def _(pair):
            values = []
            for row in range(ROWS_B):
                index = pair * ROWS_B + row
                hidden = norm_relu(zb[index]).astype(BF16)
                hb[index] = hidden
                values.append(conv_in(0, index, hidden))
            return tally(64, *values)

        blocks = wi.shape[0]
        for block in range(blocks):
            layer, step = 3 + 3 * block, 3 + block
            moments(layer, bn_i[block], count_b, (lambda: prepare_block(2)) if block == 0 else None)

            @sweep
            def _(pair):
                norm_mid(pair, 0)
                norm_mid(pair, ROWS_B - 1)

            for side in range(2):
                exchange(step, side, m_src[side], m_dst[side])

            @sweep
            def _(pair):
                for row in range(1, ROWS_B - 1):
                    norm_mid(pair, row)
                return tally(64, conv_mid(block, pair, 1, 2))

            for side in range(2):
                settle(step, side, m_src[side], m_dst[side])

            @sweep
            def _(pair):
                rebuild_mid(pair, 0)
                rebuild_mid(pair, ROWS_B + 1)
                return tally(64, conv_mid(block, pair, 0, 1), conv_mid(block, pair, ROWS_B - 1, 1))

            moments(layer + 1, bn_m[block], count_b)

            @sweep
            def _(pair):
                values = []
                for row in range(ROWS_B):
                    index = pair * ROWS_B + row
                    values.append(mm(wo[block], norm_relu(za[index]).astype(BF16)))
                    zb[index] = values[-1]
                return tally(128, *values)

            moments(layer + 2, bn_o[block], count_b)

            def finish(index):
                return jnp.maximum(affine(zb[index]) + hb[index].astype(F32), 0.0)

            if block < blocks - 1:
                @sweep
                def _(pair):
                    values = []
                    for row in range(ROWS_B):
                        index = pair * ROWS_B + row
                        hidden = finish(index).astype(BF16)
                        hb[index] = hidden
                        values.append(conv_in(block + 1, index, hidden))
                    return tally(64, *values)
            else:
                def out_copy(pair):
                    return pltpu.make_async_copy(ov.at[pair], out_hbm.at[pl.ds(2 * pair, 2)], out_sem.at[pair])

                @sweep
                def _(pair):
                    for row in range(ROWS_B):
                        value = finish(pair * ROWS_B + row)
                        for image in range(2):
                            ov[pair, image, row] = value[:, image * 128:(image + 1) * 128].T.astype(BF16)
                    out_copy(pair).start()

                @sweep
                def _(pair):
                    out_copy(pair).wait()

    def forward(images, w_a, bn_a, w_down, bn_down, w_in, bn_in, w_mid, bn_mid, w_out, bn_out):
        images_count = images.shape[0]
        pairs = images_count // 2
        x = jnp.transpose(images, (0, 1, 3, 2))
        layers = w_a.shape[0] + 1 + 3 * w_in.shape[0]
        steps = 3 + w_in.shape[0]
        vmem = pl.BlockSpec(memory_space=pltpu.VMEM)
        hbm = pl.BlockSpec(memory_space=pl.ANY)
        dma = pltpu.SemaphoreType.DMA
        return pl.pallas_call(
            kernel,
            out_shape=jax.ShapeDtypeStruct((images_count, ROWS_B, 128, 128), BF16),
            in_specs=[hbm] + [vmem] * 10,
            out_specs=hbm,
            scratch_shapes=[
                pltpu.VMEM((w_a.shape[0], 128, 512), BF16),
                pltpu.VMEM((128, 384), BF16),
                pltpu.VMEM((w_in.shape[0], 128, 768), BF16),
                pltpu.VMEM((w_in.shape[0], 128, 64), BF16),
                pltpu.VMEM((pairs, 2, ROWS_A, 32, LANES), BF16),
                pltpu.VMEM((2, images_count, 32, LANES), BF16),
                pltpu.VMEM((pairs, ROWS_A + 2, 128, LANES), BF16),
                pltpu.VMEM((pairs, ROWS_B + 2, 192, LANES), BF16),
                pltpu.VMEM((pairs * ROWS_A, 64, LANES), F32),
                pltpu.VMEM((pairs * ROWS_B, 128, LANES), F32),
                pltpu.VMEM((pairs * ROWS_B, 128, LANES), BF16),
                pltpu.VMEM((pairs, 2, ROWS_B, 128, 128), BF16),
                pltpu.VMEM((2, 128, 128), F32),
                pltpu.VMEM((2, 128, 128), F32),
                pltpu.VMEM((layers, groups, 16, 128), F32),
                dma((pairs,)), dma((pairs,)), dma((steps, 2)), dma((steps, 2)),
                dma((layers, groups)), dma((layers, groups)),
            ],
            compiler_params=pltpu.CompilerParams(
                collective_id=0, has_side_effects=True, vmem_limit_bytes=67043328),
            name="conv_stack",
        )(x, w_a, bn_a, w_down, bn_down, jnp.transpose(w_in, (0, 2, 1)), bn_in, w_mid, bn_mid, w_out, bn_out)

    act_spec = P("dp", "sp", None, None)
    return jax.shard_map(forward, mesh=mesh, in_specs=(act_spec,) + (P(),) * 10, out_specs=act_spec, check_vma=False)
```

```python
import functools

import jax
import jax.numpy as jnp
from jax import lax
from jax.experimental import pallas as pl
from jax.experimental.pallas import tpu as pltpu
from jax.sharding import PartitionSpec as P

NORM_EPS = 1e-5
MESH = pl.DeviceIdType.MESH
F32 = jnp.float32
BF16 = jnp.bfloat16
ROWS_A = 8
ROWS_B = 4
UNROLL = 4
LANES = 256


def solution(mesh):
    groups = mesh.shape["sp"]

    def kernel(x_hbm, raw_a, bn_a, raw_d, bn_d, wi, bn_i, raw_m, bn_m, raw_o, bn_o, out_hbm,
               perm, wa, wd, wm, wo, xv, xh, hs, us, za, zb, hb, ov, acc, ab, stat,
               x_sem, out_sem, halo_send, halo_recv, stat_send, stat_recv):
        pairs = xv.shape[0]
        me = lax.axis_index("sp")
        count_a = float(2 * pairs * ROWS_A * LANES * groups)
        count_b = float(2 * pairs * ROWS_B * 128 * groups)

        def sweep(body, before=None, after=None):
            @pl.loop(0, pairs // UNROLL)
            def _(step):
                if before is not None:
                    before(step)
                sums = [body(step * UNROLL + part) for part in range(UNROLL)]
                if after is not None:
                    after(step)
                if sums[0] is not None:
                    channels = sums[0].shape[1]
                    acc[:, 0:channels] += sum(sums[1:], sums[0])

        def x_copy(pair):
            return pltpu.make_async_copy(x_hbm.at[pl.ds(2 * pair, 2)], xv.at[pair], x_sem.at[pair])

        @sweep
        def _(pair):
            x_copy(pair).start()

        barrier = pltpu.get_barrier_semaphore()
        for hop in range(1, groups):
            pl.semaphore_signal(barrier, inc=1, device_id={"sp": lax.rem(me + hop, groups)}, device_id_type=MESH)
        pl.semaphore_wait(barrier, groups - 1)

        def halo_copy(step, side, chunk, refs, peer):
            src, dst = refs[side](chunk * UNROLL)
            return pltpu.make_async_remote_copy(
                src_ref=src, dst_ref=dst, send_sem=halo_send.at[step, side, chunk],
                recv_sem=halo_recv.at[step, side, chunk], device_id={"sp": peer}, device_id_type=MESH)

        def exchange(step, refs, chunk, sides=(0, 1)):
            for side in sides:
                @pl.when(me < groups - 1 if side == 0 else me > 0)
                def _():
                    halo_copy(step, side, chunk, refs, me + 1 if side == 0 else me - 1).start()

        def settle(step, refs, chunk, sides=(0, 1)):
            for side in sides:
                @pl.when(me > 0 if side == 0 else me < groups - 1)
                def _():
                    halo_copy(step, side, chunk, refs, me - 1 if side == 0 else me + 1).wait_recv()

                @pl.when(me < groups - 1 if side == 0 else me > 0)
                def _():
                    halo_copy(step, side, chunk, refs, me + 1 if side == 0 else me - 1).wait_send()

        def x_part(row, slot):
            return lambda pair: (x_hbm.at[pl.ds(2 * pair, 2 * UNROLL), row], xh.at[slot, pl.ds(2 * pair, 2 * UNROLL)])

        def h_part(row, slot):
            return lambda pair: (hs.at[pl.ds(pair, UNROLL), row, 32:96], hs.at[pl.ds(pair, UNROLL), slot, 32:96])

        def u_part(row, slot):
            return lambda pair: (us.at[pl.ds(pair, UNROLL), row, 64:128], us.at[pl.ds(pair, UNROLL), slot, 64:128])

        x_refs = (x_part(ROWS_A - 1, 0), x_part(0, 1))
        h_refs = (h_part(ROWS_A, 0), h_part(1, ROWS_A + 1))
        u_refs = (u_part(ROWS_B, 0), u_part(1, ROWS_B + 1))

        @pl.loop(0, pairs // UNROLL)
        def _(chunk):
            exchange(0, x_refs, chunk)

        @pl.when(me == 0)
        def _():
            xh[0] = jnp.zeros(xh.shape[1:], BF16)

            @sweep
            def _(pair):
                hs[pair, 0] = jnp.zeros(hs.shape[2:], BF16)
                us[pair, 0] = jnp.zeros(us.shape[2:], BF16)

        @pl.when(me == groups - 1)
        def _():
            xh[1] = jnp.zeros(xh.shape[1:], BF16)

            @sweep
            def _(pair):
                hs[pair, ROWS_A + 1] = jnp.zeros(hs.shape[2:], BF16)
                us[pair, ROWS_B + 1] = jnp.zeros(us.shape[2:], BF16)

        def turn(block):
            return block.astype(F32).T.astype(BF16)

        def prepare_a(layer):
            for row in range(4):
                lines = []
                for plane in range(4):
                    tiles = []
                    for out_row in range(2):
                        for phase in range(2):
                            high, wide = row - out_row, plane - phase
                            inside = 0 <= high < 3 and 0 <= wide < 3
                            tiles.append(raw_a[layer, high, wide].astype(F32) if inside else jnp.zeros((32, 32), F32))
                    lines.append(jnp.concatenate(tiles, axis=1))
                wa[layer, :, 128 * row:128 * row + 128] = turn(jnp.concatenate(lines, axis=0))

        def prepare_down():
            for high in range(3):
                lines = [jnp.zeros((32, 128), BF16)] + [raw_d[high, wide] for wide in range(3)]
                wd[:, 128 * high:128 * high + 128] = turn(jnp.concatenate(lines, axis=0))

        def prepare_block(block):
            lines = []
            for row in range(4):
                for wide in range(3):
                    tiles = []
                    for out_row in range(2):
                        high = row - out_row
                        inside = 0 <= high < 3
                        tiles.append(raw_m[block, high, wide].astype(F32) if inside else jnp.zeros((64, 64), F32))
                    lines.append(jnp.concatenate(tiles, axis=1))
            for part in range(6):
                wm[block, :, 128 * part:128 * part + 128] = turn(jnp.concatenate(lines[2 * part:2 * part + 2], axis=0))
            wo[block] = turn(raw_o[block])

        def shift(value, step):
            lane = lax.broadcasted_iota(jnp.int32, (value.shape[0], 128), 1)
            edge = 0 if step == 1 else 127
            halves = []
            for half in range(2):
                moved = pltpu.roll(value[:, half * 128:(half + 1) * 128], step % 128, 1)
                halves.append(jnp.where(lane == edge, 0.0, moved))
            return jnp.concatenate(halves, axis=1)

        def put_planes(pair, row, even, odd, centre=True):
            hs[pair, row, 0:32] = shift(odd, 1).astype(BF16)
            if centre:
                hs[pair, row, 32:64] = even.astype(BF16)
                hs[pair, row, 64:96] = odd.astype(BF16)
            hs[pair, row, 96:128] = shift(even, -1).astype(BF16)

        def put_mid(pair, row, value, centre=True):
            us[pair, row, 0:64] = shift(value, 1).astype(BF16)
            if centre:
                us[pair, row, 64:128] = value.astype(BF16)
            us[pair, row, 128:192] = shift(value, -1).astype(BF16)

        def rebuild_a(pair, row):
            both = hs[pair, row, 32:96].astype(F32)
            put_planes(pair, row, both[0:32], both[32:64], centre=False)

        def rebuild_mid(pair, row):
            put_mid(pair, row, us[pair, row, 64:128].astype(F32), centre=False)

        def clear():
            acc[...] = jnp.zeros(acc.shape, F32)

        def tally(channels, *values):
            total, square = 0.0, 0.0
            for value in values:
                for half in range(2):
                    for row in range(0, value.shape[0], channels):
                        piece = value[row:row + channels, half * 128:(half + 1) * 128]
                        total, square = total + piece, square + piece * piece
            return jnp.stack([total, square])

        def moments(layer, params, count, during=None):
            channels = params.shape[1]
            for part in range(2):
                turned = jnp.concatenate([acc[part, 0:channels]] * (128 // channels), axis=0).T.reshape(16, 8, 128)
                stat[layer, me, 8 * part:8 * part + 8] = jnp.sum(turned, axis=0)
            copies = []
            for hop in range(1, groups):
                copies.append(pltpu.make_async_remote_copy(
                    src_ref=stat.at[layer, me], dst_ref=stat.at[layer, me],
                    send_sem=stat_send.at[layer, hop], recv_sem=stat_recv.at[layer, hop],
                    device_id={"sp": lax.rem(me + hop, groups)}, device_id_type=MESH))
            for copy in copies:
                copy.start()
            clear()
            if during is not None:
                during()
            for hop in range(1, groups):
                origin = lax.rem(me + groups - hop, groups)
                pltpu.make_async_remote_copy(
                    src_ref=stat.at[layer, origin], dst_ref=stat.at[layer, origin],
                    send_sem=stat_send.at[layer, hop], recv_sem=stat_recv.at[layer, hop],
                    device_id={"sp": origin}, device_id_type=MESH).wait_recv()
            for copy in copies:
                copy.wait_send()
            total = stat[layer, 0]
            for origin in range(1, groups):
                total = total + stat[layer, origin]

            def fold(block):
                return jnp.sum(block, axis=0, keepdims=True) / count

            mean, square = fold(total[0:8]), fold(total[8:16])
            var = square - mean * mean
            wide = jnp.concatenate([params] * (128 // channels), axis=1)
            scale = wide[0:1] * lax.rsqrt(var + NORM_EPS)
            bias = wide[1:2] - mean * scale
            ab[0] = jnp.broadcast_to(scale, (128, 128)).T
            ab[1] = jnp.broadcast_to(bias, (128, 128)).T

        def affine(value):
            rows = value.shape[0]
            scale, bias = ab[0, 0:rows], ab[1, 0:rows]
            return jnp.concatenate(
                [value[:, :128] * scale + bias, value[:, 128:] * scale + bias], axis=1)

        def norm_relu(value):
            return jnp.maximum(affine(value), 0.0)

        def mm(left, right):
            return jnp.dot(left, right, preferred_element_type=F32)

        clear()
        for layer in range(wa.shape[0]):
            prepare_a(layer)

        lane_in = lax.broadcasted_iota(jnp.int32, (LANES, LANES), 0)
        lane_out = lax.broadcasted_iota(jnp.int32, (LANES, LANES), 1)
        source = jnp.where(lane_out < 128, 2 * lane_out, 2 * lane_out - (LANES - 1))
        perm[...] = jnp.where(lane_in == source, 1.0, 0.0).astype(BF16)

        def split_rows(first, second, pair, row):
            put_planes(pair, row, jnp.concatenate([first[:, :128], second[:, :128]], axis=1),
                       jnp.concatenate([first[:, 128:], second[:, 128:]], axis=1))

        def conv_a(layer, pair, row, rows):
            window = hs[pair, row:row + rows + 2].reshape((rows + 2) * 128, LANES)
            value = mm(wa[layer, 0:64 * rows, 0:128 * (rows + 2)], window)
            za[pl.ds(pair * ROWS_A + row, rows)] = value.reshape(rows, 64, LANES)
            return value

        def norm_a(pair, row):
            value = norm_relu(za[pair * ROWS_A + row])
            put_planes(pair, row + 1, value[0:32], value[32:64])

        @sweep
        def _(pair):
            x_copy(pair).wait()
            both = mm(xv[pair].reshape(2 * ROWS_A * 32, LANES), perm[...]).reshape(2, ROWS_A, 32, LANES)
            for row in range(ROWS_A):
                split_rows(both[0, row], both[1, row], pair, row + 1)
            return tally(32, *[conv_a(0, pair, row, 2) for row in range(1, ROWS_A - 1, 2)])

        @functools.partial(sweep, before=lambda chunk: settle(0, x_refs, chunk))
        def _(pair):
            both = mm(xh[:, pl.ds(2 * pair, 2)].reshape(4 * 32, LANES), perm[...]).reshape(2, 2, 32, LANES)
            split_rows(both[0, 0], both[0, 1], pair, 0)
            split_rows(both[1, 0], both[1, 1], pair, ROWS_A + 1)
            return tally(32, conv_a(0, pair, 0, 1), conv_a(0, pair, ROWS_A - 1, 1))

        moments(0, bn_a[0], count_a, prepare_down)

        @functools.partial(sweep, after=lambda chunk: exchange(1, h_refs, chunk))
        def _(pair):
            norm_a(pair, 0)
            norm_a(pair, ROWS_A - 1)

        @sweep
        def _(pair):
            for row in range(1, ROWS_A - 1):
                norm_a(pair, row)
            return tally(32, *[conv_a(1, pair, row, 2) for row in range(1, ROWS_A - 1, 2)])

        @functools.partial(sweep, before=lambda chunk: settle(1, h_refs, chunk))
        def _(pair):
            rebuild_a(pair, 0)
            rebuild_a(pair, ROWS_A + 1)
            return tally(32, conv_a(1, pair, 0, 1), conv_a(1, pair, ROWS_A - 1, 1))

        moments(1, bn_a[1], count_a, lambda: prepare_block(0))

        def conv_down(pair, row):
            window = hs[pair, 2 * row + 1:2 * row + 4].reshape(384, LANES)
            value = mm(wd[...], window)
            zb[pair * ROWS_B + row] = value
            return value

        @functools.partial(sweep, after=lambda chunk: exchange(2, h_refs, chunk, (1,)))
        def _(pair):
            norm_a(pair, 0)

        @sweep
        def _(pair):
            for row in range(1, ROWS_A):
                norm_a(pair, row)
            return tally(128, *[conv_down(pair, row) for row in range(ROWS_B - 1)])

        @functools.partial(sweep, before=lambda chunk: settle(2, h_refs, chunk, (1,)))
        def _(pair):
            rebuild_a(pair, ROWS_A + 1)
            return tally(128, conv_down(pair, ROWS_B - 1))

        moments(2, bn_d[...], count_b, lambda: prepare_block(1))

        def conv_in(block, index, hidden):
            value = mm(wi[block], hidden)
            za[index] = value
            return value

        def conv_mid(block, pair, row, rows):
            window = us[pair, row:row + rows + 2].reshape((rows + 2) * 192, LANES)
            value = mm(wm[block, 0:64 * rows, 0:192 * (rows + 2)], window)
            za[pl.ds(pair * ROWS_B + row, rows)] = value.reshape(rows, 64, LANES)
            return value

        def norm_mid(pair, row):
            put_mid(pair, row + 1, norm_relu(za[pair * ROWS_B + row]))

        @sweep
        def _(pair):
            values = []
            for row in range(ROWS_B):
                index = pair * ROWS_B + row
                hidden = norm_relu(zb[index]).astype(BF16)
                hb[index] = hidden
                values.append(conv_in(0, index, hidden))
            return tally(64, *values)

        blocks = wi.shape[0]
        for block in range(blocks):
            layer, step = 3 + 3 * block, 3 + block
            moments(layer, bn_i[block], count_b, (lambda: prepare_block(2)) if block == 0 else None)

            @functools.partial(sweep, after=lambda chunk: exchange(step, u_refs, chunk))
            def _(pair):
                norm_mid(pair, 0)
                norm_mid(pair, ROWS_B - 1)

            @sweep
            def _(pair):
                for row in range(1, ROWS_B - 1):
                    norm_mid(pair, row)
                return tally(64, conv_mid(block, pair, 1, 2))

            @functools.partial(sweep, before=lambda chunk: settle(step, u_refs, chunk))
            def _(pair):
                rebuild_mid(pair, 0)
                rebuild_mid(pair, ROWS_B + 1)
                return tally(64, conv_mid(block, pair, 0, 1), conv_mid(block, pair, ROWS_B - 1, 1))

            moments(layer + 1, bn_m[block], count_b)

            @sweep
            def _(pair):
                values = []
                for row in range(ROWS_B):
                    index = pair * ROWS_B + row
                    values.append(mm(wo[block], norm_relu(za[index]).astype(BF16)))
                    zb[index] = values[-1]
                return tally(128, *values)

            moments(layer + 2, bn_o[block], count_b)

            def finish(index):
                return jnp.maximum(affine(zb[index]) + hb[index].astype(F32), 0.0)

            if block < blocks - 1:
                @sweep
                def _(pair):
                    values = []
                    for row in range(ROWS_B):
                        index = pair * ROWS_B + row
                        hidden = finish(index).astype(BF16)
                        hb[index] = hidden
                        values.append(conv_in(block + 1, index, hidden))
                    return tally(64, *values)
            else:
                def out_copy(pair):
                    return pltpu.make_async_copy(ov.at[pair], out_hbm.at[pl.ds(2 * pair, 2)], out_sem.at[pair])

                @sweep
                def _(pair):
                    for row in range(ROWS_B):
                        value = finish(pair * ROWS_B + row)
                        for image in range(2):
                            ov[pair, image, row] = value[:, image * 128:(image + 1) * 128].T.astype(BF16)
                    out_copy(pair).start()

                @sweep
                def _(pair):
                    out_copy(pair).wait()

    def forward(images, w_a, bn_a, w_down, bn_down, w_in, bn_in, w_mid, bn_mid, w_out, bn_out):
        images_count = images.shape[0]
        pairs = images_count // 2
        x = jnp.transpose(images, (0, 1, 3, 2))
        layers = w_a.shape[0] + 1 + 3 * w_in.shape[0]
        steps = 3 + w_in.shape[0]
        vmem = pl.BlockSpec(memory_space=pltpu.VMEM)
        hbm = pl.BlockSpec(memory_space=pl.ANY)
        dma = pltpu.SemaphoreType.DMA
        return pl.pallas_call(
            kernel,
            out_shape=jax.ShapeDtypeStruct((images_count, ROWS_B, 128, 128), BF16),
            in_specs=[hbm] + [vmem] * 10,
            out_specs=hbm,
            scratch_shapes=[
                pltpu.VMEM((LANES, LANES), BF16),
                pltpu.VMEM((w_a.shape[0], 128, 512), BF16),
                pltpu.VMEM((128, 384), BF16),
                pltpu.VMEM((w_in.shape[0], 128, 768), BF16),
                pltpu.VMEM((w_in.shape[0], 128, 64), BF16),
                pltpu.VMEM((pairs, 2, ROWS_A, 32, LANES), BF16),
                pltpu.VMEM((2, images_count, 32, LANES), BF16),
                pltpu.VMEM((pairs, ROWS_A + 2, 128, LANES), BF16),
                pltpu.VMEM((pairs, ROWS_B + 2, 192, LANES), BF16),
                pltpu.VMEM((pairs * ROWS_A, 64, LANES), F32),
                pltpu.VMEM((pairs * ROWS_B, 128, LANES), F32),
                pltpu.VMEM((pairs * ROWS_B, 128, LANES), BF16),
                pltpu.VMEM((pairs, 2, ROWS_B, 128, 128), BF16),
                pltpu.VMEM((2, 128, 128), F32),
                pltpu.VMEM((2, 128, 128), F32),
                pltpu.VMEM((layers, groups, 16, 128), F32),
                dma((pairs,)), dma((pairs,)), dma((steps, 2, pairs // UNROLL)), dma((steps, 2, pairs // UNROLL)),
                dma((layers, groups)), dma((layers, groups)),
            ],
            compiler_params=pltpu.CompilerParams(
                collective_id=0, has_side_effects=True, vmem_limit_bytes=67043328),
            name="conv_stack",
        )(x, w_a, bn_a, w_down, bn_down, jnp.transpose(w_in, (0, 2, 1)), bn_in, w_mid, bn_mid, w_out, bn_out)

    act_spec = P("dp", "sp", None, None)
    return jax.shard_map(forward, mesh=mesh, in_specs=(act_spec,) + (P(),) * 10, out_specs=act_spec, check_vma=False)
```

```python
import functools

import jax
import jax.numpy as jnp
from jax import lax
from jax.experimental import pallas as pl
from jax.experimental.pallas import tpu as pltpu
from jax.sharding import PartitionSpec as P

NORM_EPS = 1e-5
MESH = pl.DeviceIdType.MESH
F32 = jnp.float32
BF16 = jnp.bfloat16
ROWS_A = 8
ROWS_B = 4
UNROLL = 4
LANES = 256


def solution(mesh):
    groups = mesh.shape["sp"]

    def kernel(x_hbm, raw_a_hbm, bn_a, raw_d_hbm, bn_d, wi_hbm, bn_i, raw_m_hbm, bn_m, raw_o_hbm, bn_o, out_hbm,
               raw_a, raw_d, wi, raw_m, raw_o, w_sem,
               perm, wa, wd, wm, wo, xv, xh, hs, us, za, zb, hb, ov, acc, ab, stat,
               x_sem, out_sem, halo_send, halo_recv, stat_send, stat_recv):
        pairs = xv.shape[0]
        me = lax.axis_index("sp")
        count_a = float(2 * pairs * ROWS_A * LANES * groups)
        count_b = float(2 * pairs * ROWS_B * 128 * groups)

        def sweep(body, *later, before=None, after=None):
            @pl.loop(0, pairs // UNROLL)
            def _(step):
                if before is not None:
                    before(step)
                for stage in (body,) + later:
                    sums = [stage(step * UNROLL + part) for part in range(UNROLL)]
                if after is not None:
                    after(step)
                if sums[0] is not None:
                    channels = sums[0].shape[1]
                    acc[:, 0:channels] += sum(sums[1:], sums[0])

        def x_copy(pair):
            return pltpu.make_async_copy(x_hbm.at[pl.ds(2 * pair, 2)], xv.at[pair], x_sem.at[pair])

        @sweep
        def _(pair):
            x_copy(pair).start()

        loads = [pltpu.make_async_copy(src, dst, w_sem.at[index]) for index, (src, dst) in enumerate(
            [(raw_a_hbm, raw_a), (raw_d_hbm, raw_d), (raw_m_hbm, raw_m), (raw_o_hbm, raw_o), (wi_hbm, wi)])]
        for load in loads:
            load.start()

        barrier = pltpu.get_barrier_semaphore()
        for hop in range(1, groups):
            pl.semaphore_signal(barrier, inc=1, device_id={"sp": lax.rem(me + hop, groups)}, device_id_type=MESH)
        pl.semaphore_wait(barrier, groups - 1)

        def halo_copy(step, side, chunk, refs, peer):
            src, dst = refs[side](chunk * UNROLL)
            return pltpu.make_async_remote_copy(
                src_ref=src, dst_ref=dst, send_sem=halo_send.at[step, side, chunk],
                recv_sem=halo_recv.at[step, side, chunk], device_id={"sp": peer}, device_id_type=MESH)

        def exchange(step, refs, chunk, sides=(0, 1)):
            for side in sides:
                @pl.when(me < groups - 1 if side == 0 else me > 0)
                def _():
                    halo_copy(step, side, chunk, refs, me + 1 if side == 0 else me - 1).start()

        def settle(step, refs, chunk, sides=(0, 1)):
            for side in sides:
                @pl.when(me > 0 if side == 0 else me < groups - 1)
                def _():
                    halo_copy(step, side, chunk, refs, me - 1 if side == 0 else me + 1).wait_recv()

                @pl.when(me < groups - 1 if side == 0 else me > 0)
                def _():
                    halo_copy(step, side, chunk, refs, me + 1 if side == 0 else me - 1).wait_send()

        def x_part(row, slot):
            return lambda pair: (x_hbm.at[pl.ds(2 * pair, 2 * UNROLL), row], xh.at[slot, pl.ds(2 * pair, 2 * UNROLL)])

        def h_part(row, slot):
            return lambda pair: (hs.at[pl.ds(pair, UNROLL), row, 32:96], hs.at[pl.ds(pair, UNROLL), slot, 32:96])

        def u_part(row, slot):
            return lambda pair: (us.at[pl.ds(pair, UNROLL), row, 64:128], us.at[pl.ds(pair, UNROLL), slot, 64:128])

        x_refs = (x_part(ROWS_A - 1, 0), x_part(0, 1))
        h_refs = (h_part(ROWS_A, 0), h_part(1, ROWS_A + 1))
        u_refs = (u_part(ROWS_B, 0), u_part(1, ROWS_B + 1))

        @pl.loop(0, pairs // UNROLL)
        def _(chunk):
            exchange(0, x_refs, chunk)

        @pl.when(me == 0)
        def _():
            xh[0] = jnp.zeros(xh.shape[1:], BF16)

            @sweep
            def _(pair):
                hs[pair, 0] = jnp.zeros(hs.shape[2:], BF16)
                us[pair, 0] = jnp.zeros(us.shape[2:], BF16)

        @pl.when(me == groups - 1)
        def _():
            xh[1] = jnp.zeros(xh.shape[1:], BF16)

            @sweep
            def _(pair):
                hs[pair, ROWS_A + 1] = jnp.zeros(hs.shape[2:], BF16)
                us[pair, ROWS_B + 1] = jnp.zeros(us.shape[2:], BF16)

        def turn(block):
            return block.astype(F32).T.astype(BF16)

        def prepare_a(layer):
            for row in range(4):
                lines = []
                for plane in range(4):
                    tiles = []
                    for out_row in range(2):
                        for phase in range(2):
                            high, wide = row - out_row, plane - phase
                            inside = 0 <= high < 3 and 0 <= wide < 3
                            tiles.append(raw_a[layer, high, wide].astype(F32) if inside else jnp.zeros((32, 32), F32))
                    lines.append(jnp.concatenate(tiles, axis=1))
                wa[layer, :, 128 * row:128 * row + 128] = turn(jnp.concatenate(lines, axis=0))

        def prepare_down():
            for high in range(3):
                lines = [jnp.zeros((32, 128), BF16)] + [raw_d[high, wide] for wide in range(3)]
                wd[:, 128 * high:128 * high + 128] = turn(jnp.concatenate(lines, axis=0))

        def prepare_block(block):
            lines = []
            for row in range(4):
                for wide in range(3):
                    tiles = []
                    for out_row in range(2):
                        high = row - out_row
                        inside = 0 <= high < 3
                        tiles.append(raw_m[block, high, wide].astype(F32) if inside else jnp.zeros((64, 64), F32))
                    lines.append(jnp.concatenate(tiles, axis=1))
            for part in range(6):
                wm[block, :, 128 * part:128 * part + 128] = turn(jnp.concatenate(lines[2 * part:2 * part + 2], axis=0))
            wo[block] = turn(raw_o[block])

        def shift(value, step):
            lane = lax.broadcasted_iota(jnp.int32, (value.shape[0], 128), 1)
            edge = 0 if step == 1 else 127
            halves = []
            for half in range(2):
                moved = pltpu.roll(value[:, half * 128:(half + 1) * 128], step % 128, 1)
                halves.append(jnp.where(lane == edge, 0.0, moved))
            return jnp.concatenate(halves, axis=1)

        def put_planes(pair, row, even, odd, centre=True):
            hs[pair, row, 0:32] = shift(odd, 1).astype(BF16)
            if centre:
                hs[pair, row, 32:64] = even.astype(BF16)
                hs[pair, row, 64:96] = odd.astype(BF16)
            hs[pair, row, 96:128] = shift(even, -1).astype(BF16)

        def put_mid(pair, row, value, centre=True):
            us[pair, row, 0:64] = shift(value, 1).astype(BF16)
            if centre:
                us[pair, row, 64:128] = value.astype(BF16)
            us[pair, row, 128:192] = shift(value, -1).astype(BF16)

        def rebuild_a(pair, row):
            both = hs[pair, row, 32:96].astype(F32)
            put_planes(pair, row, both[0:32], both[32:64], centre=False)

        def rebuild_mid(pair, row):
            put_mid(pair, row, us[pair, row, 64:128].astype(F32), centre=False)

        def clear():
            acc[...] = jnp.zeros(acc.shape, F32)

        def tally(channels, *values):
            total, square = 0.0, 0.0
            for value in values:
                for half in range(2):
                    for row in range(0, value.shape[0], channels):
                        piece = value[row:row + channels, half * 128:(half + 1) * 128]
                        total, square = total + piece, square + piece * piece
            return jnp.stack([total, square])

        def moments(layer, params, count, during=None):
            channels = params.shape[1]
            for part in range(2):
                turned = jnp.concatenate([acc[part, 0:channels]] * (128 // channels), axis=0).T.reshape(16, 8, 128)
                stat[layer, me, 8 * part:8 * part + 8] = jnp.sum(turned, axis=0)
            copies = []
            for hop in range(1, groups):
                copies.append(pltpu.make_async_remote_copy(
                    src_ref=stat.at[layer, me], dst_ref=stat.at[layer, me],
                    send_sem=stat_send.at[layer, hop], recv_sem=stat_recv.at[layer, hop],
                    device_id={"sp": lax.rem(me + hop, groups)}, device_id_type=MESH))
            for copy in copies:
                copy.start()
            clear()
            if during is not None:
                during()
            for hop in range(1, groups):
                origin = lax.rem(me + groups - hop, groups)
                pltpu.make_async_remote_copy(
                    src_ref=stat.at[layer, origin], dst_ref=stat.at[layer, origin],
                    send_sem=stat_send.at[layer, hop], recv_sem=stat_recv.at[layer, hop],
                    device_id={"sp": origin}, device_id_type=MESH).wait_recv()
            for copy in copies:
                copy.wait_send()
            total = stat[layer, 0]
            for origin in range(1, groups):
                total = total + stat[layer, origin]

            def fold(block):
                return jnp.sum(block, axis=0, keepdims=True) / count

            mean, square = fold(total[0:8]), fold(total[8:16])
            var = square - mean * mean
            wide = jnp.concatenate([params] * (128 // channels), axis=1)
            scale = wide[0:1] * lax.rsqrt(var + NORM_EPS)
            bias = wide[1:2] - mean * scale
            ab[0] = jnp.broadcast_to(scale, (128, 128)).T
            ab[1] = jnp.broadcast_to(bias, (128, 128)).T

        def affine(value):
            rows = value.shape[0]
            scale, bias = ab[0, 0:rows], ab[1, 0:rows]
            return jnp.concatenate(
                [value[:, :128] * scale + bias, value[:, 128:] * scale + bias], axis=1)

        def norm_relu(value):
            return jnp.maximum(affine(value), 0.0)

        def mm(left, right):
            return jnp.dot(left, right, preferred_element_type=F32)

        clear()
        loads[0].wait()
        prepare_a(0)

        lane_in = lax.broadcasted_iota(jnp.int32, (LANES, LANES), 0)
        lane_out = lax.broadcasted_iota(jnp.int32, (LANES, LANES), 1)
        source = jnp.where(lane_out < 128, 2 * lane_out, 2 * lane_out - (LANES - 1))
        perm[...] = jnp.where(lane_in == source, 1.0, 0.0).astype(BF16)

        def split_rows(first, second, pair, row):
            put_planes(pair, row, jnp.concatenate([first[:, :128], second[:, :128]], axis=1),
                       jnp.concatenate([first[:, 128:], second[:, 128:]], axis=1))

        def conv_a(layer, pair, row, rows):
            window = hs[pair, row:row + rows + 2].reshape((rows + 2) * 128, LANES)
            value = mm(wa[layer, 0:64 * rows, 0:128 * (rows + 2)], window)
            za[pl.ds(pair * ROWS_A + row, rows)] = value.reshape(rows, 64, LANES)
            return value

        def norm_a(pair, row):
            value = norm_relu(za[pair * ROWS_A + row])
            put_planes(pair, row + 1, value[0:32], value[32:64])

        def planes(pair):
            x_copy(pair).wait()
            both = mm(xv[pair].reshape(2 * ROWS_A * 32, LANES), perm[...]).reshape(2, ROWS_A, 32, LANES)
            for row in range(ROWS_A):
                split_rows(both[0, row], both[1, row], pair, row + 1)

        def inner_a(layer):
            return lambda pair: tally(32, *[conv_a(layer, pair, row, 2) for row in range(1, ROWS_A - 1, 2)])

        def outer_a(layer):
            return lambda pair: tally(32, conv_a(layer, pair, 0, 1), conv_a(layer, pair, ROWS_A - 1, 1))

        sweep(planes, inner_a(0))

        def halo_planes(pair):
            both = mm(xh[:, pl.ds(2 * pair, 2)].reshape(4 * 32, LANES), perm[...]).reshape(2, 2, 32, LANES)
            split_rows(both[0, 0], both[0, 1], pair, 0)
            split_rows(both[1, 0], both[1, 1], pair, ROWS_A + 1)

        sweep(halo_planes, outer_a(0), before=lambda chunk: settle(0, x_refs, chunk))

        def second_weights():
            for load in loads[1:]:
                load.wait()
            prepare_a(1)

        moments(0, bn_a[0], count_a, second_weights)

        @functools.partial(sweep, after=lambda chunk: exchange(1, h_refs, chunk))
        def _(pair):
            norm_a(pair, 0)
            norm_a(pair, ROWS_A - 1)

        def norm_inner(pair):
            for row in range(1, ROWS_A - 1):
                norm_a(pair, row)

        sweep(norm_inner, inner_a(1))

        def rebuild_both(pair):
            rebuild_a(pair, 0)
            rebuild_a(pair, ROWS_A + 1)

        sweep(rebuild_both, outer_a(1), before=lambda chunk: settle(1, h_refs, chunk))

        moments(1, bn_a[1], count_a, prepare_down)

        def conv_down(pair, row):
            window = hs[pair, 2 * row + 1:2 * row + 4].reshape(384, LANES)
            value = mm(wd[...], window)
            zb[pair * ROWS_B + row] = value
            return value

        @functools.partial(sweep, after=lambda chunk: exchange(2, h_refs, chunk, (1,)))
        def _(pair):
            norm_a(pair, 0)

        def norm_below(pair):
            for row in range(1, ROWS_A):
                norm_a(pair, row)

        sweep(norm_below, lambda pair: tally(128, *[conv_down(pair, row) for row in range(ROWS_B - 1)]))
        sweep(lambda pair: rebuild_a(pair, ROWS_A + 1), lambda pair: tally(128, conv_down(pair, ROWS_B - 1)),
              before=lambda chunk: settle(2, h_refs, chunk, (1,)))

        moments(2, bn_d[...], count_b, lambda: prepare_block(0))

        def conv_in(block, index):
            value = mm(wi[block], hb[index])
            za[index] = value
            return value

        def conv_mid(block, pair, row, rows):
            window = us[pair, row:row + rows + 2].reshape((rows + 2) * 192, LANES)
            value = mm(wm[block, 0:64 * rows, 0:192 * (rows + 2)], window)
            za[pl.ds(pair * ROWS_B + row, rows)] = value.reshape(rows, 64, LANES)
            return value

        def norm_mid(pair, row):
            put_mid(pair, row + 1, norm_relu(za[pair * ROWS_B + row]))

        def all_in(block):
            return lambda pair: tally(64, *[conv_in(block, pair * ROWS_B + row) for row in range(ROWS_B)])

        def first_hidden(pair):
            for row in range(ROWS_B):
                index = pair * ROWS_B + row
                hb[index] = norm_relu(zb[index]).astype(BF16)

        sweep(first_hidden, all_in(0))

        blocks = wi.shape[0]
        for block in range(blocks):
            layer, step = 3 + 3 * block, 3 + block
            moments(layer, bn_i[block], count_b, (lambda: prepare_block(block + 1)) if block < blocks - 1 else None)

            @functools.partial(sweep, after=lambda chunk: exchange(step, u_refs, chunk))
            def _(pair):
                norm_mid(pair, 0)
                norm_mid(pair, ROWS_B - 1)

            def mid_inner(pair):
                for row in range(1, ROWS_B - 1):
                    norm_mid(pair, row)

            def mid_outer(pair):
                rebuild_mid(pair, 0)
                rebuild_mid(pair, ROWS_B + 1)

            sweep(mid_inner, lambda pair: tally(64, conv_mid(block, pair, 1, 2)))
            sweep(mid_outer,
                  lambda pair: tally(64, conv_mid(block, pair, 0, 1), conv_mid(block, pair, ROWS_B - 1, 1)),
                  before=lambda chunk: settle(step, u_refs, chunk))

            moments(layer + 1, bn_m[block], count_b)

            @sweep
            def _(pair):
                values = []
                for row in range(ROWS_B):
                    index = pair * ROWS_B + row
                    values.append(mm(wo[block], norm_relu(za[index]).astype(BF16)))
                    zb[index] = values[-1]
                return tally(128, *values)

            moments(layer + 2, bn_o[block], count_b)

            def finish(index):
                return jnp.maximum(affine(zb[index]) + hb[index].astype(F32), 0.0)

            if block < blocks - 1:
                def next_hidden(pair):
                    for row in range(ROWS_B):
                        index = pair * ROWS_B + row
                        hb[index] = finish(index).astype(BF16)

                sweep(next_hidden, all_in(block + 1))
            else:
                def out_copy(pair):
                    return pltpu.make_async_copy(ov.at[pair], out_hbm.at[pl.ds(2 * pair, 2)], out_sem.at[pair])

                @sweep
                def _(pair):
                    for row in range(ROWS_B):
                        value = finish(pair * ROWS_B + row)
                        for image in range(2):
                            ov[pair, image, row] = value[:, image * 128:(image + 1) * 128].T.astype(BF16)
                    out_copy(pair).start()

                @sweep
                def _(pair):
                    out_copy(pair).wait()

    def forward(images, w_a, bn_a, w_down, bn_down, w_in, bn_in, w_mid, bn_mid, w_out, bn_out):
        images_count = images.shape[0]
        pairs = images_count // 2
        x = jnp.transpose(images, (0, 1, 3, 2))
        layers = w_a.shape[0] + 1 + 3 * w_in.shape[0]
        steps = 3 + w_in.shape[0]
        vmem = pl.BlockSpec(memory_space=pltpu.VMEM)
        hbm = pl.BlockSpec(memory_space=pl.ANY)
        dma = pltpu.SemaphoreType.DMA
        return pl.pallas_call(
            kernel,
            out_shape=jax.ShapeDtypeStruct((images_count, ROWS_B, 128, 128), BF16),
            in_specs=[hbm] + [hbm, vmem] * 5,
            out_specs=hbm,
            scratch_shapes=[
                pltpu.VMEM(w_a.shape, BF16), pltpu.VMEM(w_down.shape, BF16), pltpu.VMEM((w_in.shape[0], 64, 128), BF16),
                pltpu.VMEM(w_mid.shape, BF16), pltpu.VMEM(w_out.shape, BF16), dma((5,)),
                pltpu.VMEM((LANES, LANES), BF16),
                pltpu.VMEM((w_a.shape[0], 128, 512), BF16),
                pltpu.VMEM((128, 384), BF16),
                pltpu.VMEM((w_in.shape[0], 128, 768), BF16),
                pltpu.VMEM((w_in.shape[0], 128, 64), BF16),
                pltpu.VMEM((pairs, 2, ROWS_A, 32, LANES), BF16),
                pltpu.VMEM((2, images_count, 32, LANES), BF16),
                pltpu.VMEM((pairs, ROWS_A + 2, 128, LANES), BF16),
                pltpu.VMEM((pairs, ROWS_B + 2, 192, LANES), BF16),
                pltpu.VMEM((pairs * ROWS_A, 64, LANES), F32),
                pltpu.VMEM((pairs * ROWS_B, 128, LANES), F32),
                pltpu.VMEM((pairs * ROWS_B, 128, LANES), BF16),
                pltpu.VMEM((pairs, 2, ROWS_B, 128, 128), BF16),
                pltpu.VMEM((2, 128, 128), F32),
                pltpu.VMEM((2, 128, 128), F32),
                pltpu.VMEM((layers, groups, 16, 128), F32),
                dma((pairs,)), dma((pairs,)), dma((steps, 2, pairs // UNROLL)), dma((steps, 2, pairs // UNROLL)),
                dma((layers, groups)), dma((layers, groups)),
            ],
            compiler_params=pltpu.CompilerParams(
                collective_id=0, has_side_effects=True, vmem_limit_bytes=67043328),
            name="conv_stack",
        )(x, w_a, bn_a, w_down, bn_down, jnp.transpose(w_in, (0, 2, 1)), bn_in, w_mid, bn_mid, w_out, bn_out)

    act_spec = P("dp", "sp", None, None)
    return jax.shard_map(forward, mesh=mesh, in_specs=(act_spec,) + (P(),) * 10, out_specs=act_spec, check_vma=False)
```

```python
import functools

import jax
import jax.numpy as jnp
from jax import lax
from jax.experimental import pallas as pl
from jax.experimental.pallas import tpu as pltpu
from jax.sharding import PartitionSpec as P

NORM_EPS = 1e-5
MESH = pl.DeviceIdType.MESH
F32 = jnp.float32
BF16 = jnp.bfloat16
ROWS_A = 8
ROWS_B = 4
UNROLL = 4
LANES = 256


def solution(mesh):
    groups = mesh.shape["sp"]

    def kernel(x_hbm, raw_a_hbm, bn_a, raw_d_hbm, bn_d, wi_hbm, bn_i, raw_m_hbm, bn_m, raw_o_hbm, bn_o, out_hbm,
               raw_a, raw_d, wi, raw_m, raw_o, w_sem,
               perm, wa, wd, wm, wo, xv, xh, hs, us, za, zb, hb, ov, acc, ab, stat,
               x_sem, out_sem, halo_send, halo_recv, zh, early_send, early_recv, stat_send, stat_recv):
        pairs = xv.shape[0]
        me = lax.axis_index("sp")
        count_a = float(2 * pairs * ROWS_A * LANES * groups)
        count_b = float(2 * pairs * ROWS_B * 128 * groups)

        def sweep(body, *later, before=None, after=None, first=0):
            @pl.loop(first, pairs // UNROLL)
            def _(step):
                if before is not None:
                    before(step)
                for stage in (body,) + later:
                    sums = [stage(step * UNROLL + part) for part in range(UNROLL)]
                if after is not None:
                    after(step)
                if sums[0] is not None:
                    channels = sums[0].shape[1]
                    acc[:, 0:channels] += sum(sums[1:], sums[0])

        def x_copy(pair):
            return pltpu.make_async_copy(x_hbm.at[pl.ds(2 * pair, 2)], xv.at[pair], x_sem.at[pair])

        @sweep
        def _(pair):
            x_copy(pair).start()

        loads = [pltpu.make_async_copy(src, dst, w_sem.at[index]) for index, (src, dst) in enumerate(
            [(raw_a_hbm, raw_a), (raw_d_hbm, raw_d), (raw_m_hbm, raw_m), (raw_o_hbm, raw_o), (wi_hbm, wi)])]
        for load in loads:
            load.start()

        barrier = pltpu.get_barrier_semaphore()
        for hop in range(1, groups):
            pl.semaphore_signal(barrier, inc=1, device_id={"sp": lax.rem(me + hop, groups)}, device_id_type=MESH)
        pl.semaphore_wait(barrier, groups - 1)

        def halo_copy(step, side, chunk, refs, peer):
            src, dst = refs[side](chunk * UNROLL)
            return pltpu.make_async_remote_copy(
                src_ref=src, dst_ref=dst, send_sem=halo_send.at[step, side, chunk],
                recv_sem=halo_recv.at[step, side, chunk], device_id={"sp": peer}, device_id_type=MESH)

        def exchange(step, refs, chunk, sides=(0, 1)):
            for side in sides:
                @pl.when(me < groups - 1 if side == 0 else me > 0)
                def _():
                    halo_copy(step, side, chunk, refs, me + 1 if side == 0 else me - 1).start()

        def settle(step, refs, chunk, sides=(0, 1)):
            for side in sides:
                @pl.when(me > 0 if side == 0 else me < groups - 1)
                def _():
                    halo_copy(step, side, chunk, refs, me - 1 if side == 0 else me + 1).wait_recv()

                @pl.when(me < groups - 1 if side == 0 else me > 0)
                def _():
                    halo_copy(step, side, chunk, refs, me + 1 if side == 0 else me - 1).wait_send()

        def x_part(row, slot):
            return lambda pair: (x_hbm.at[pl.ds(2 * pair, 2 * UNROLL), row], xh.at[slot, pl.ds(2 * pair, 2 * UNROLL)])

        def h_part(row, slot):
            return lambda pair: (hs.at[pl.ds(pair, UNROLL), row, 32:96], hs.at[pl.ds(pair, UNROLL), slot, 32:96])

        def u_part(row, slot):
            return lambda pair: (us.at[pl.ds(pair, UNROLL), row, 64:128], us.at[pl.ds(pair, UNROLL), slot, 64:128])

        def early_copy(step, side, part, rows, peer):
            return pltpu.make_async_remote_copy(
                src_ref=za.at[part * rows + (rows - 1 if side == 0 else 0)], dst_ref=zh.at[step, side, part],
                send_sem=early_send.at[step, side, part], recv_sem=early_recv.at[step, side, part],
                device_id={"sp": peer}, device_id_type=MESH)

        def early(step, rows, sides=(0, 1)):
            for side in sides:
                @pl.when(me < groups - 1 if side == 0 else me > 0)
                def _():
                    for part in range(UNROLL):
                        early_copy(step, side, part, rows, me + 1 if side == 0 else me - 1).start()

        def settle_early(step, rows, put, sides=(0, 1)):
            for side in sides:
                @pl.when(me > 0 if side == 0 else me < groups - 1)
                def _():
                    for part in range(UNROLL):
                        early_copy(step, side, part, rows, me - 1 if side == 0 else me + 1).wait_recv()
                    for part in range(UNROLL):
                        put(part, 0 if side == 0 else rows + 1, norm_relu(zh[step, side, part]))

                @pl.when(me < groups - 1 if side == 0 else me > 0)
                def _():
                    for part in range(UNROLL):
                        early_copy(step, side, part, rows, me + 1 if side == 0 else me - 1).wait_send()

        def first_chunk(*stages):
            for stage in stages:
                sums = [stage(part) for part in range(UNROLL)]
            if sums[0] is not None:
                acc[:, 0:sums[0].shape[1]] += sum(sums[1:], sums[0])

        x_refs = (x_part(ROWS_A - 1, 0), x_part(0, 1))
        h_refs = (h_part(ROWS_A, 0), h_part(1, ROWS_A + 1))
        u_refs = (u_part(ROWS_B, 0), u_part(1, ROWS_B + 1))

        @pl.loop(0, pairs // UNROLL)
        def _(chunk):
            exchange(0, x_refs, chunk)

        @pl.when(me == 0)
        def _():
            xh[0] = jnp.zeros(xh.shape[1:], BF16)

            @sweep
            def _(pair):
                hs[pair, 0] = jnp.zeros(hs.shape[2:], BF16)
                us[pair, 0] = jnp.zeros(us.shape[2:], BF16)

        @pl.when(me == groups - 1)
        def _():
            xh[1] = jnp.zeros(xh.shape[1:], BF16)

            @sweep
            def _(pair):
                hs[pair, ROWS_A + 1] = jnp.zeros(hs.shape[2:], BF16)
                us[pair, ROWS_B + 1] = jnp.zeros(us.shape[2:], BF16)

        def turn(block):
            return block.astype(F32).T.astype(BF16)

        def prepare_a(layer):
            for row in range(4):
                lines = []
                for plane in range(4):
                    tiles = []
                    for out_row in range(2):
                        for phase in range(2):
                            high, wide = row - out_row, plane - phase
                            inside = 0 <= high < 3 and 0 <= wide < 3
                            tiles.append(raw_a[layer, high, wide].astype(F32) if inside else jnp.zeros((32, 32), F32))
                    lines.append(jnp.concatenate(tiles, axis=1))
                wa[layer, :, 128 * row:128 * row + 128] = turn(jnp.concatenate(lines, axis=0))

        def prepare_down():
            for high in range(3):
                lines = [jnp.zeros((32, 128), BF16)] + [raw_d[high, wide] for wide in range(3)]
                wd[:, 128 * high:128 * high + 128] = turn(jnp.concatenate(lines, axis=0))

        def prepare_block(block):
            lines = []
            for row in range(4):
                for wide in range(3):
                    tiles = []
                    for out_row in range(2):
                        high = row - out_row
                        inside = 0 <= high < 3
                        tiles.append(raw_m[block, high, wide].astype(F32) if inside else jnp.zeros((64, 64), F32))
                    lines.append(jnp.concatenate(tiles, axis=1))
            for part in range(6):
                wm[block, :, 128 * part:128 * part + 128] = turn(jnp.concatenate(lines[2 * part:2 * part + 2], axis=0))
            wo[block] = turn(raw_o[block])

        def shift(value, step):
            lane = lax.broadcasted_iota(jnp.int32, (value.shape[0], 128), 1)
            edge = 0 if step == 1 else 127
            halves = []
            for half in range(2):
                moved = pltpu.roll(value[:, half * 128:(half + 1) * 128], step % 128, 1)
                halves.append(jnp.where(lane == edge, 0.0, moved))
            return jnp.concatenate(halves, axis=1)

        def put_planes(pair, row, even, odd, centre=True):
            hs[pair, row, 0:32] = shift(odd, 1).astype(BF16)
            if centre:
                hs[pair, row, 32:64] = even.astype(BF16)
                hs[pair, row, 64:96] = odd.astype(BF16)
            hs[pair, row, 96:128] = shift(even, -1).astype(BF16)

        def put_mid(pair, row, value, centre=True):
            us[pair, row, 0:64] = shift(value, 1).astype(BF16)
            if centre:
                us[pair, row, 64:128] = value.astype(BF16)
            us[pair, row, 128:192] = shift(value, -1).astype(BF16)

        def rebuild_a(pair, row):
            both = hs[pair, row, 32:96].astype(F32)
            put_planes(pair, row, both[0:32], both[32:64], centre=False)

        def rebuild_mid(pair, row):
            put_mid(pair, row, us[pair, row, 64:128].astype(F32), centre=False)

        def clear():
            acc[...] = jnp.zeros(acc.shape, F32)

        def tally(channels, *values):
            total, square = 0.0, 0.0
            for value in values:
                for half in range(2):
                    for row in range(0, value.shape[0], channels):
                        piece = value[row:row + channels, half * 128:(half + 1) * 128]
                        total, square = total + piece, square + piece * piece
            return jnp.stack([total, square])

        def moments(layer, params, count, during=None, early=None):
            channels = params.shape[1]
            for part in range(2):
                turned = jnp.concatenate([acc[part, 0:channels]] * (128 // channels), axis=0).T.reshape(16, 8, 128)
                stat[layer, me, 8 * part:8 * part + 8] = jnp.sum(turned, axis=0)
            copies = []
            for hop in range(1, groups):
                copies.append(pltpu.make_async_remote_copy(
                    src_ref=stat.at[layer, me], dst_ref=stat.at[layer, me],
                    send_sem=stat_send.at[layer, hop], recv_sem=stat_recv.at[layer, hop],
                    device_id={"sp": lax.rem(me + hop, groups)}, device_id_type=MESH))
            for copy in copies:
                copy.start()
            if early is not None:
                early()
            clear()
            if during is not None:
                during()
            for hop in range(1, groups):
                origin = lax.rem(me + groups - hop, groups)
                pltpu.make_async_remote_copy(
                    src_ref=stat.at[layer, origin], dst_ref=stat.at[layer, origin],
                    send_sem=stat_send.at[layer, hop], recv_sem=stat_recv.at[layer, hop],
                    device_id={"sp": origin}, device_id_type=MESH).wait_recv()
            for copy in copies:
                copy.wait_send()
            total = stat[layer, 0]
            for origin in range(1, groups):
                total = total + stat[layer, origin]

            def fold(block):
                return jnp.sum(block, axis=0, keepdims=True) / count

            mean, square = fold(total[0:8]), fold(total[8:16])
            var = square - mean * mean
            wide = jnp.concatenate([params] * (128 // channels), axis=1)
            scale = wide[0:1] * lax.rsqrt(var + NORM_EPS)
            bias = wide[1:2] - mean * scale
            ab[0] = jnp.broadcast_to(scale, (128, 128)).T
            ab[1] = jnp.broadcast_to(bias, (128, 128)).T

        def affine(value):
            rows = value.shape[0]
            scale, bias = ab[0, 0:rows], ab[1, 0:rows]
            return jnp.concatenate(
                [value[:, :128] * scale + bias, value[:, 128:] * scale + bias], axis=1)

        def norm_relu(value):
            return jnp.maximum(affine(value), 0.0)

        def mm(left, right):
            return jnp.dot(left, right, preferred_element_type=F32)

        clear()
        loads[0].wait()
        prepare_a(0)

        lane_in = lax.broadcasted_iota(jnp.int32, (LANES, LANES), 0)
        lane_out = lax.broadcasted_iota(jnp.int32, (LANES, LANES), 1)
        source = jnp.where(lane_out < 128, 2 * lane_out, 2 * lane_out - (LANES - 1))
        perm[...] = jnp.where(lane_in == source, 1.0, 0.0).astype(BF16)

        def split_rows(first, second, pair, row):
            put_planes(pair, row, jnp.concatenate([first[:, :128], second[:, :128]], axis=1),
                       jnp.concatenate([first[:, 128:], second[:, 128:]], axis=1))

        def conv_a(layer, pair, row, rows):
            window = hs[pair, row:row + rows + 2].reshape((rows + 2) * 128, LANES)
            value = mm(wa[layer, 0:64 * rows, 0:128 * (rows + 2)], window)
            za[pl.ds(pair * ROWS_A + row, rows)] = value.reshape(rows, 64, LANES)
            return value

        def norm_a(pair, row):
            value = norm_relu(za[pair * ROWS_A + row])
            put_planes(pair, row + 1, value[0:32], value[32:64])

        def planes(pair):
            x_copy(pair).wait()
            both = mm(xv[pair].reshape(2 * ROWS_A * 32, LANES), perm[...]).reshape(2, ROWS_A, 32, LANES)
            for row in range(ROWS_A):
                split_rows(both[0, row], both[1, row], pair, row + 1)

        def inner_a(layer):
            return lambda pair: tally(32, *[conv_a(layer, pair, row, 2) for row in range(1, ROWS_A - 1, 2)])

        def outer_a(layer):
            return lambda pair: tally(32, conv_a(layer, pair, 0, 1), conv_a(layer, pair, ROWS_A - 1, 1))

        sweep(planes, inner_a(0))

        def halo_planes(pair):
            both = mm(xh[:, pl.ds(2 * pair, 2)].reshape(4 * 32, LANES), perm[...]).reshape(2, 2, 32, LANES)
            split_rows(both[0, 0], both[0, 1], pair, 0)
            split_rows(both[1, 0], both[1, 1], pair, ROWS_A + 1)

        sweep(halo_planes, outer_a(0), before=lambda chunk: settle(0, x_refs, chunk))

        def second_weights():
            for load in loads[1:]:
                load.wait()
            prepare_a(1)

        moments(0, bn_a[0], count_a, second_weights, lambda: early(1, ROWS_A))

        def norm_edges(pair):
            norm_a(pair, 0)
            norm_a(pair, ROWS_A - 1)

        def put_edge(pair, slot, value):
            put_planes(pair, slot, value[0:32], value[32:64])

        sweep(norm_edges, after=lambda chunk: exchange(1, h_refs, chunk), first=1)
        first_chunk(norm_edges)

        def norm_inner(pair):
            for row in range(1, ROWS_A - 1):
                norm_a(pair, row)

        sweep(norm_inner, inner_a(1))

        def rebuild_both(pair):
            rebuild_a(pair, 0)
            rebuild_a(pair, ROWS_A + 1)

        settle_early(1, ROWS_A, put_edge)
        first_chunk(outer_a(1))
        sweep(rebuild_both, outer_a(1), before=lambda chunk: settle(1, h_refs, chunk), first=1)

        moments(1, bn_a[1], count_a, prepare_down, lambda: early(2, ROWS_A, (1,)))

        def conv_down(pair, row):
            window = hs[pair, 2 * row + 1:2 * row + 4].reshape(384, LANES)
            value = mm(wd[...], window)
            zb[pair * ROWS_B + row] = value
            return value

        sweep(lambda pair: norm_a(pair, 0), after=lambda chunk: exchange(2, h_refs, chunk, (1,)), first=1)
        first_chunk(lambda pair: norm_a(pair, 0))

        def norm_below(pair):
            for row in range(1, ROWS_A):
                norm_a(pair, row)

        sweep(norm_below, lambda pair: tally(128, *[conv_down(pair, row) for row in range(ROWS_B - 1)]))

        def down_edge(pair):
            return tally(128, conv_down(pair, ROWS_B - 1))

        settle_early(2, ROWS_A, put_edge, (1,))
        first_chunk(down_edge)
        sweep(lambda pair: rebuild_a(pair, ROWS_A + 1), down_edge,
              before=lambda chunk: settle(2, h_refs, chunk, (1,)), first=1)

        moments(2, bn_d[...], count_b, lambda: prepare_block(0))

        def conv_in(block, index):
            value = mm(wi[block], hb[index])
            za[index] = value
            return value

        def conv_mid(block, pair, row, rows):
            window = us[pair, row:row + rows + 2].reshape((rows + 2) * 192, LANES)
            value = mm(wm[block, 0:64 * rows, 0:192 * (rows + 2)], window)
            za[pl.ds(pair * ROWS_B + row, rows)] = value.reshape(rows, 64, LANES)
            return value

        def norm_mid(pair, row):
            put_mid(pair, row + 1, norm_relu(za[pair * ROWS_B + row]))

        def all_in(block):
            return lambda pair: tally(64, *[conv_in(block, pair * ROWS_B + row) for row in range(ROWS_B)])

        def first_hidden(pair):
            for row in range(ROWS_B):
                index = pair * ROWS_B + row
                hb[index] = norm_relu(zb[index]).astype(BF16)

        sweep(first_hidden, all_in(0))

        blocks = wi.shape[0]
        for block in range(blocks):
            layer, step = 3 + 3 * block, 3 + block
            moments(layer, bn_i[block], count_b, (lambda: prepare_block(block + 1)) if block < blocks - 1 else None,
                    lambda: early(step, ROWS_B))

            def mid_edges(pair):
                norm_mid(pair, 0)
                norm_mid(pair, ROWS_B - 1)

            def mid_conv(pair):
                return tally(64, conv_mid(block, pair, 0, 1), conv_mid(block, pair, ROWS_B - 1, 1))

            sweep(mid_edges, after=lambda chunk: exchange(step, u_refs, chunk), first=1)
            first_chunk(mid_edges)

            def mid_inner(pair):
                for row in range(1, ROWS_B - 1):
                    norm_mid(pair, row)

            def mid_outer(pair):
                rebuild_mid(pair, 0)
                rebuild_mid(pair, ROWS_B + 1)

            sweep(mid_inner, lambda pair: tally(64, conv_mid(block, pair, 1, 2)))
            settle_early(step, ROWS_B, put_mid)
            first_chunk(mid_conv)
            sweep(mid_outer, mid_conv, before=lambda chunk: settle(step, u_refs, chunk), first=1)

            moments(layer + 1, bn_m[block], count_b)

            @sweep
            def _(pair):
                values = []
                for row in range(ROWS_B):
                    index = pair * ROWS_B + row
                    values.append(mm(wo[block], norm_relu(za[index]).astype(BF16)))
                    zb[index] = values[-1]
                return tally(128, *values)

            moments(layer + 2, bn_o[block], count_b)

            def finish(index):
                return jnp.maximum(affine(zb[index]) + hb[index].astype(F32), 0.0)

            if block < blocks - 1:
                def next_hidden(pair):
                    for row in range(ROWS_B):
                        index = pair * ROWS_B + row
                        hb[index] = finish(index).astype(BF16)

                sweep(next_hidden, all_in(block + 1))
            else:
                def out_copy(pair):
                    return pltpu.make_async_copy(ov.at[pair], out_hbm.at[pl.ds(2 * pair, 2)], out_sem.at[pair])

                @sweep
                def _(pair):
                    for row in range(ROWS_B):
                        value = finish(pair * ROWS_B + row)
                        for image in range(2):
                            ov[pair, image, row] = value[:, image * 128:(image + 1) * 128].T.astype(BF16)
                    out_copy(pair).start()

                @sweep
                def _(pair):
                    out_copy(pair).wait()

    def forward(images, w_a, bn_a, w_down, bn_down, w_in, bn_in, w_mid, bn_mid, w_out, bn_out):
        images_count = images.shape[0]
        pairs = images_count // 2
        x = jnp.transpose(images, (0, 1, 3, 2))
        layers = w_a.shape[0] + 1 + 3 * w_in.shape[0]
        steps = 3 + w_in.shape[0]
        vmem = pl.BlockSpec(memory_space=pltpu.VMEM)
        hbm = pl.BlockSpec(memory_space=pl.ANY)
        dma = pltpu.SemaphoreType.DMA
        return pl.pallas_call(
            kernel,
            out_shape=jax.ShapeDtypeStruct((images_count, ROWS_B, 128, 128), BF16),
            in_specs=[hbm] + [hbm, vmem] * 5,
            out_specs=hbm,
            scratch_shapes=[
                pltpu.VMEM(w_a.shape, BF16), pltpu.VMEM(w_down.shape, BF16), pltpu.VMEM((w_in.shape[0], 64, 128), BF16),
                pltpu.VMEM(w_mid.shape, BF16), pltpu.VMEM(w_out.shape, BF16), dma((5,)),
                pltpu.VMEM((LANES, LANES), BF16),
                pltpu.VMEM((w_a.shape[0], 128, 512), BF16),
                pltpu.VMEM((128, 384), BF16),
                pltpu.VMEM((w_in.shape[0], 128, 768), BF16),
                pltpu.VMEM((w_in.shape[0], 128, 64), BF16),
                pltpu.VMEM((pairs, 2, ROWS_A, 32, LANES), BF16),
                pltpu.VMEM((2, images_count, 32, LANES), BF16),
                pltpu.VMEM((pairs, ROWS_A + 2, 128, LANES), BF16),
                pltpu.VMEM((pairs, ROWS_B + 2, 192, LANES), BF16),
                pltpu.VMEM((pairs * ROWS_A, 64, LANES), F32),
                pltpu.VMEM((pairs * ROWS_B, 128, LANES), F32),
                pltpu.VMEM((pairs * ROWS_B, 128, LANES), BF16),
                pltpu.VMEM((pairs, 2, ROWS_B, 128, 128), BF16),
                pltpu.VMEM((2, 128, 128), F32),
                pltpu.VMEM((2, 128, 128), F32),
                pltpu.VMEM((layers, groups, 16, 128), F32),
                dma((pairs,)), dma((pairs,)), dma((steps, 2, pairs // UNROLL)), dma((steps, 2, pairs // UNROLL)),
                pltpu.VMEM((steps, 2, UNROLL, 64, LANES), F32), dma((steps, 2, UNROLL)), dma((steps, 2, UNROLL)),
                dma((layers, groups)), dma((layers, groups)),
            ],
            compiler_params=pltpu.CompilerParams(
                collective_id=0, has_side_effects=True, vmem_limit_bytes=67043328),
            name="conv_stack",
        )(x, w_a, bn_a, w_down, bn_down, jnp.transpose(w_in, (0, 2, 1)), bn_in, w_mid, bn_mid, w_out, bn_out)

    act_spec = P("dp", "sp", None, None)
    return jax.shard_map(forward, mesh=mesh, in_specs=(act_spec,) + (P(),) * 10, out_specs=act_spec, check_vma=False)
```

```python
import functools

import jax
import jax.numpy as jnp
from jax import lax
from jax.experimental import pallas as pl
from jax.experimental.pallas import tpu as pltpu
from jax.sharding import PartitionSpec as P

NORM_EPS = 1e-5
MESH = pl.DeviceIdType.MESH
F32 = jnp.float32
BF16 = jnp.bfloat16
ROWS_A = 8
ROWS_B = 4
UNROLL = 4
LAST_STEPS = 4
LANES = 256
HALF = 128
MID = 64
CIN = 32
THREE = 96
TRIPLE = 192
DOWN_K = 384
BAND_A = 512
BAND_B = 768
FOUR = 4
SUB = 8
PAIR_SUB = 16


def solution(mesh):
    groups = mesh.shape["sp"]

    def kernel(x_hbm, raw_a_hbm, bn_a, raw_d_hbm, bn_d, wi_hbm, bn_i, raw_m_hbm, bn_m, raw_o_hbm, bn_o,
               h_hbm, u_hbm, scale_out, weight_out,
               raw_a, raw_d, wi, raw_m, raw_o, w_sem,
               perm, wa, wd, wm, wo, xv, xh, hs, us, za, zb, hb, ub, acc, ab, stat,
               x_sem, out_sem, halo_send, halo_recv, zh, early_send, early_recv, stat_send, stat_recv):
        pairs = xv.shape[0]
        me = lax.axis_index("sp")
        count_a = float(2 * pairs * ROWS_A * LANES * groups)
        count_b = float(2 * pairs * ROWS_B * HALF * groups)

        def sweep(body, *later, before=None, after=None, first=0):
            @pl.loop(first, pairs // UNROLL)
            def _(step):
                if before is not None:
                    before(step)
                for stage in (body,) + later:
                    sums = [stage(step * UNROLL + part) for part in range(UNROLL)]
                if after is not None:
                    after(step)
                if sums[0] is not None:
                    channels = sums[0].shape[1]
                    acc[:, 0:channels] += sum(sums[1:], sums[0])

        def x_copy(pair):
            return pltpu.make_async_copy(x_hbm.at[pl.ds(2 * pair, 2)], xv.at[pair], x_sem.at[pair])

        @sweep
        def _(pair):
            x_copy(pair).start()

        loads = [pltpu.make_async_copy(src, dst, w_sem.at[index]) for index, (src, dst) in enumerate(
            [(raw_a_hbm, raw_a), (raw_d_hbm, raw_d), (raw_m_hbm, raw_m), (raw_o_hbm, raw_o), (wi_hbm, wi)])]
        for load in loads:
            load.start()

        barrier = pltpu.get_barrier_semaphore()
        for hop in range(1, groups):
            pl.semaphore_signal(barrier, inc=1, device_id={"sp": lax.rem(me + hop, groups)}, device_id_type=MESH)
        pl.semaphore_wait(barrier, groups - 1)

        def halo_copy(step, side, chunk, refs, peer):
            src, dst = refs[side](chunk * UNROLL)
            return pltpu.make_async_remote_copy(
                src_ref=src, dst_ref=dst, send_sem=halo_send.at[step, side, chunk],
                recv_sem=halo_recv.at[step, side, chunk], device_id={"sp": peer}, device_id_type=MESH)

        def exchange(step, refs, chunk, sides=(0, 1)):
            for side in sides:
                @pl.when(me < groups - 1 if side == 0 else me > 0)
                def _():
                    halo_copy(step, side, chunk, refs, me + 1 if side == 0 else me - 1).start()

        def settle(step, refs, chunk, sides=(0, 1)):
            for side in sides:
                @pl.when(me > 0 if side == 0 else me < groups - 1)
                def _():
                    halo_copy(step, side, chunk, refs, me - 1 if side == 0 else me + 1).wait_recv()

                @pl.when(me < groups - 1 if side == 0 else me > 0)
                def _():
                    halo_copy(step, side, chunk, refs, me + 1 if side == 0 else me - 1).wait_send()

        def x_part(row, slot):
            return lambda pair: (x_hbm.at[pl.ds(2 * pair, 2 * UNROLL), row], xh.at[slot, pl.ds(2 * pair, 2 * UNROLL)])

        def h_part(row, slot):
            return lambda pair: (hs.at[pl.ds(pair, UNROLL), row, CIN:THREE], hs.at[pl.ds(pair, UNROLL), slot, CIN:THREE])

        def u_part(row, slot):
            return lambda pair: (us.at[pl.ds(pair, UNROLL), row, MID:HALF], us.at[pl.ds(pair, UNROLL), slot, MID:HALF])

        def early_copy(step, side, part, rows, peer):
            return pltpu.make_async_remote_copy(
                src_ref=za.at[part * rows + (rows - 1 if side == 0 else 0)], dst_ref=zh.at[step, side, part],
                send_sem=early_send.at[step, side, part], recv_sem=early_recv.at[step, side, part],
                device_id={"sp": peer}, device_id_type=MESH)

        def early(step, rows, sides=(0, 1)):
            for side in sides:
                @pl.when(me < groups - 1 if side == 0 else me > 0)
                def _():
                    for part in range(UNROLL):
                        early_copy(step, side, part, rows, me + 1 if side == 0 else me - 1).start()

        def settle_early(step, rows, put, sides=(0, 1)):
            for side in sides:
                @pl.when(me > 0 if side == 0 else me < groups - 1)
                def _():
                    for part in range(UNROLL):
                        early_copy(step, side, part, rows, me - 1 if side == 0 else me + 1).wait_recv()
                    for part in range(UNROLL):
                        put(part, 0 if side == 0 else rows + 1, norm_relu(zh[step, side, part]))

                @pl.when(me < groups - 1 if side == 0 else me > 0)
                def _():
                    for part in range(UNROLL):
                        early_copy(step, side, part, rows, me + 1 if side == 0 else me - 1).wait_send()

        def first_chunk(*stages):
            for stage in stages:
                sums = [stage(part) for part in range(UNROLL)]
            if sums[0] is not None:
                acc[:, 0:sums[0].shape[1]] += sum(sums[1:], sums[0])

        x_refs = (x_part(ROWS_A - 1, 0), x_part(0, 1))
        h_refs = (h_part(ROWS_A, 0), h_part(1, ROWS_A + 1))
        u_refs = (u_part(ROWS_B, 0), u_part(1, ROWS_B + 1))

        @pl.loop(0, pairs // UNROLL)
        def _(chunk):
            exchange(0, x_refs, chunk)

        @pl.when(me == 0)
        def _():
            xh[0] = jnp.zeros(xh.shape[1:], BF16)

            @sweep
            def _(pair):
                hs[pair, 0] = jnp.zeros(hs.shape[2:], BF16)
                us[pair, 0] = jnp.zeros(us.shape[2:], BF16)

        @pl.when(me == groups - 1)
        def _():
            xh[1] = jnp.zeros(xh.shape[1:], BF16)

            @sweep
            def _(pair):
                hs[pair, ROWS_A + 1] = jnp.zeros(hs.shape[2:], BF16)
                us[pair, ROWS_B + 1] = jnp.zeros(us.shape[2:], BF16)

        def turn(block):
            return block.astype(F32).T.astype(BF16)

        def prepare_a(layer):
            for row in range(FOUR):
                lines = []
                for plane in range(FOUR):
                    tiles = []
                    for out_row in range(2):
                        for phase in range(2):
                            high, wide = row - out_row, plane - phase
                            inside = 0 <= high < 3 and 0 <= wide < 3
                            tiles.append(raw_a[layer, high, wide].astype(F32) if inside else jnp.zeros((CIN, CIN), F32))
                    lines.append(jnp.concatenate(tiles, axis=1))
                wa[layer, :, HALF * row:HALF * row + HALF] = turn(jnp.concatenate(lines, axis=0))

        def prepare_down():
            for high in range(3):
                lines = [jnp.zeros((CIN, HALF), BF16)] + [raw_d[high, wide] for wide in range(3)]
                wd[:, HALF * high:HALF * high + HALF] = turn(jnp.concatenate(lines, axis=0))

        def prepare_block(block):
            lines = []
            for row in range(FOUR):
                for wide in range(3):
                    tiles = []
                    for out_row in range(2):
                        high = row - out_row
                        inside = 0 <= high < 3
                        tiles.append(raw_m[block, high, wide].astype(F32) if inside else jnp.zeros((MID, MID), F32))
                    lines.append(jnp.concatenate(tiles, axis=1))
            for part in range(6):
                wm[block, :, HALF * part:HALF * part + HALF] = turn(jnp.concatenate(lines[2 * part:2 * part + 2], axis=0))
            wo[block] = turn(raw_o[block])

        def shift(value, step):
            lane = lax.broadcasted_iota(jnp.int32, (value.shape[0], HALF), 1)
            edge = 0 if step == 1 else 127
            halves = []
            for half in range(2):
                moved = pltpu.roll(value[:, half * HALF:(half + 1) * HALF], step % HALF, 1)
                halves.append(jnp.where(lane == edge, 0.0, moved))
            return jnp.concatenate(halves, axis=1)

        def put_planes(pair, row, even, odd, centre=True):
            hs[pair, row, 0:CIN] = shift(odd, 1).astype(BF16)
            if centre:
                hs[pair, row, CIN:MID] = even.astype(BF16)
                hs[pair, row, MID:THREE] = odd.astype(BF16)
            hs[pair, row, THREE:HALF] = shift(even, -1).astype(BF16)

        def put_mid(pair, row, value, centre=True):
            us[pair, row, 0:MID] = shift(value, 1).astype(BF16)
            if centre:
                us[pair, row, MID:HALF] = value.astype(BF16)
            us[pair, row, HALF:TRIPLE] = shift(value, -1).astype(BF16)

        def rebuild_a(pair, row):
            both = hs[pair, row, CIN:THREE].astype(F32)
            put_planes(pair, row, both[0:CIN], both[CIN:MID], centre=False)

        def rebuild_mid(pair, row):
            put_mid(pair, row, us[pair, row, MID:HALF].astype(F32), centre=False)

        def clear():
            acc[...] = jnp.zeros(acc.shape, F32)

        def tally(channels, *values):
            total, square = 0.0, 0.0
            for value in values:
                for half in range(2):
                    for row in range(0, value.shape[0], channels):
                        piece = value[row:row + channels, half * HALF:(half + 1) * HALF]
                        total, square = total + piece, square + piece * piece
            return jnp.stack([total, square])

        def moments(layer, params, count, during=None, early=None):
            channels = params.shape[1]
            for part in range(2):
                turned = jnp.concatenate([acc[part, 0:channels]] * (HALF // channels), axis=0).T.reshape(PAIR_SUB, SUB, HALF)
                stat[layer, me, SUB * part:SUB * part + SUB] = jnp.sum(turned, axis=0)
            copies = []
            for hop in range(1, groups):
                copies.append(pltpu.make_async_remote_copy(
                    src_ref=stat.at[layer, me], dst_ref=stat.at[layer, me],
                    send_sem=stat_send.at[layer, hop], recv_sem=stat_recv.at[layer, hop],
                    device_id={"sp": lax.rem(me + hop, groups)}, device_id_type=MESH))
            for copy in copies:
                copy.start()
            if early is not None:
                early()
            clear()
            if during is not None:
                during()
            for hop in range(1, groups):
                origin = lax.rem(me + groups - hop, groups)
                pltpu.make_async_remote_copy(
                    src_ref=stat.at[layer, origin], dst_ref=stat.at[layer, origin],
                    send_sem=stat_send.at[layer, hop], recv_sem=stat_recv.at[layer, hop],
                    device_id={"sp": origin}, device_id_type=MESH).wait_recv()
            for copy in copies:
                copy.wait_send()
            total = stat[layer, 0]
            for origin in range(1, groups):
                total = total + stat[layer, origin]

            def fold(block):
                return jnp.sum(block, axis=0, keepdims=True) / count

            mean, square = fold(total[0:SUB]), fold(total[SUB:PAIR_SUB])
            var = square - mean * mean
            wide = jnp.concatenate([params] * (HALF // channels), axis=1)
            scale = wide[0:1] * lax.rsqrt(var + NORM_EPS)
            bias = wide[1:2] - mean * scale
            ab[0] = jnp.broadcast_to(scale, (HALF, HALF)).T
            ab[1] = jnp.broadcast_to(bias, (HALF, HALF)).T

        def affine(value):
            rows = value.shape[0]
            scale, bias = ab[0, 0:rows], ab[1, 0:rows]
            return jnp.concatenate(
                [value[:, :HALF] * scale + bias, value[:, HALF:] * scale + bias], axis=1)

        def norm_relu(value):
            return jnp.maximum(affine(value), 0.0)

        def mm(left, right):
            return jnp.dot(left, right, preferred_element_type=F32)

        clear()
        loads[0].wait()
        prepare_a(0)

        lane_in = lax.broadcasted_iota(jnp.int32, (LANES, LANES), 0)
        lane_out = lax.broadcasted_iota(jnp.int32, (LANES, LANES), 1)
        source = jnp.where(lane_out < HALF, 2 * lane_out, 2 * lane_out - (LANES - 1))
        perm[...] = jnp.where(lane_in == source, 1.0, 0.0).astype(BF16)

        def split_rows(first, second, pair, row):
            put_planes(pair, row, jnp.concatenate([first[:, :HALF], second[:, :HALF]], axis=1),
                       jnp.concatenate([first[:, HALF:], second[:, HALF:]], axis=1))

        def conv_a(layer, pair, row, rows):
            window = hs[pair, row:row + rows + 2].reshape((rows + 2) * HALF, LANES)
            value = mm(wa[layer, 0:MID * rows, 0:HALF * (rows + 2)], window)
            za[pl.ds(pair * ROWS_A + row, rows)] = value.reshape(rows, MID, LANES)
            return value

        def norm_a(pair, row):
            value = norm_relu(za[pair * ROWS_A + row])
            put_planes(pair, row + 1, value[0:CIN], value[CIN:MID])

        def planes(pair):
            x_copy(pair).wait()
            both = mm(xv[pair].reshape(2 * ROWS_A * CIN, LANES), perm[...]).reshape(2, ROWS_A, CIN, LANES)
            for row in range(ROWS_A):
                split_rows(both[0, row], both[1, row], pair, row + 1)

        def inner_a(layer):
            return lambda pair: tally(CIN, *[conv_a(layer, pair, row, 2) for row in range(1, ROWS_A - 1, 2)])

        def outer_a(layer):
            return lambda pair: tally(CIN, conv_a(layer, pair, 0, 1), conv_a(layer, pair, ROWS_A - 1, 1))

        sweep(planes, inner_a(0))

        def halo_planes(pair):
            both = mm(xh[:, pl.ds(2 * pair, 2)].reshape(FOUR * CIN, LANES), perm[...]).reshape(2, 2, CIN, LANES)
            split_rows(both[0, 0], both[0, 1], pair, 0)
            split_rows(both[1, 0], both[1, 1], pair, ROWS_A + 1)

        sweep(halo_planes, outer_a(0), before=lambda chunk: settle(0, x_refs, chunk))

        def second_weights():
            for load in loads[1:]:
                load.wait()
            prepare_a(1)

        moments(0, bn_a[0], count_a, second_weights, lambda: early(1, ROWS_A))

        def norm_edges(pair):
            norm_a(pair, 0)
            norm_a(pair, ROWS_A - 1)

        def put_edge(pair, slot, value):
            put_planes(pair, slot, value[0:CIN], value[CIN:MID])

        sweep(norm_edges, after=lambda chunk: exchange(1, h_refs, chunk), first=1)
        first_chunk(norm_edges)

        def norm_inner(pair):
            for row in range(1, ROWS_A - 1):
                norm_a(pair, row)

        sweep(norm_inner, inner_a(1))

        def rebuild_both(pair):
            rebuild_a(pair, 0)
            rebuild_a(pair, ROWS_A + 1)

        settle_early(1, ROWS_A, put_edge)
        first_chunk(outer_a(1))
        sweep(rebuild_both, outer_a(1), before=lambda chunk: settle(1, h_refs, chunk), first=1)

        moments(1, bn_a[1], count_a, prepare_down, lambda: early(2, ROWS_A, (1,)))

        def conv_down(pair, row):
            window = hs[pair, 2 * row + 1:2 * row + FOUR].reshape(DOWN_K, LANES)
            value = mm(wd[...], window)
            zb[pair * ROWS_B + row] = value
            return value

        sweep(lambda pair: norm_a(pair, 0), after=lambda chunk: exchange(2, h_refs, chunk, (1,)), first=1)
        first_chunk(lambda pair: norm_a(pair, 0))

        def norm_below(pair):
            for row in range(1, ROWS_A):
                norm_a(pair, row)

        sweep(norm_below, lambda pair: tally(HALF, *[conv_down(pair, row) for row in range(ROWS_B - 1)]))

        def down_edge(pair):
            return tally(HALF, conv_down(pair, ROWS_B - 1))

        settle_early(2, ROWS_A, put_edge, (1,))
        first_chunk(down_edge)
        sweep(lambda pair: rebuild_a(pair, ROWS_A + 1), down_edge,
              before=lambda chunk: settle(2, h_refs, chunk, (1,)), first=1)

        moments(2, bn_d[...], count_b, lambda: prepare_block(0))

        def conv_in(block, index):
            value = mm(wi[block], hb[index])
            za[index] = value
            return value

        def conv_mid(block, pair, row, rows):
            window = us[pair, row:row + rows + 2].reshape((rows + 2) * TRIPLE, LANES)
            value = mm(wm[block, 0:MID * rows, 0:TRIPLE * (rows + 2)], window)
            za[pl.ds(pair * ROWS_B + row, rows)] = value.reshape(rows, MID, LANES)
            return value

        def norm_mid(pair, row):
            put_mid(pair, row + 1, norm_relu(za[pair * ROWS_B + row]))

        def all_in(block):
            return lambda pair: tally(MID, *[conv_in(block, pair * ROWS_B + row) for row in range(ROWS_B)])

        def first_hidden(pair):
            for row in range(ROWS_B):
                index = pair * ROWS_B + row
                hb[index] = norm_relu(zb[index]).astype(BF16)

        sweep(first_hidden, all_in(0))

        blocks = wi.shape[0]
        for block in range(blocks):
            layer, step = 3 + 3 * block, 3 + block
            moments(layer, bn_i[block], count_b, (lambda: prepare_block(block + 1)) if block < blocks - 1 else None,
                    lambda: early(step, ROWS_B))

            def mid_edges(pair):
                norm_mid(pair, 0)
                norm_mid(pair, ROWS_B - 1)

            def mid_conv(pair):
                return tally(MID, conv_mid(block, pair, 0, 1), conv_mid(block, pair, ROWS_B - 1, 1))

            sweep(mid_edges, after=lambda chunk: exchange(step, u_refs, chunk), first=1)
            first_chunk(mid_edges)

            def mid_inner(pair):
                for row in range(1, ROWS_B - 1):
                    norm_mid(pair, row)

            def mid_outer(pair):
                rebuild_mid(pair, 0)
                rebuild_mid(pair, ROWS_B + 1)

            sweep(mid_inner, lambda pair: tally(MID, conv_mid(block, pair, 1, 2)))
            settle_early(step, ROWS_B, put_mid)
            first_chunk(mid_conv)
            sweep(mid_outer, mid_conv, before=lambda chunk: settle(step, u_refs, chunk), first=1)

            moments(layer + 1, bn_m[block], count_b)

            last = block == blocks - 1
            if last:
                h_copy = pltpu.make_async_copy(hb, h_hbm, out_sem.at[pairs // UNROLL])
                h_copy.start()
                weight_out[...] = wo[block]

            def u_copy(chunk):
                span = pl.ds(chunk * UNROLL * ROWS_B, UNROLL * ROWS_B)
                return pltpu.make_async_copy(ub.at[span], u_hbm.at[span], out_sem.at[chunk])

            def all_out(pair):
                values = []
                for row in range(ROWS_B):
                    index = pair * ROWS_B + row
                    hidden = norm_relu(za[index]).astype(BF16)
                    values.append(mm(wo[block], hidden))
                    if last:
                        ub[index] = hidden
                    else:
                        zb[index] = values[-1]
                return tally(HALF, *values)

            sweep(all_out, after=(lambda chunk: u_copy(chunk).start()) if last else None)
            moments(layer + 2, bn_o[block], count_b)

            if not last:
                def next_hidden(pair):
                    for row in range(ROWS_B):
                        index = pair * ROWS_B + row
                        hb[index] = jnp.maximum(affine(zb[index]) + hb[index].astype(F32), 0.0).astype(BF16)

                sweep(next_hidden, all_in(block + 1))
            else:
                scale_out[...] = ab[...]
                h_copy.wait()

                @pl.loop(0, pairs // UNROLL)
                def _(chunk):
                    u_copy(chunk).wait()

    def last_kernel(h_hbm, u_hbm, scale_ref, weight_ref, out_hbm, hv, uv, ov, h_sem, u_sem, out_sem):
        chunks = h_sem.shape[0]
        span = hv.shape[0] // chunks

        def loads(chunk):
            part = pl.ds(chunk * span, span)
            return (pltpu.make_async_copy(h_hbm.at[part], hv.at[part], h_sem.at[chunk]),
                    pltpu.make_async_copy(u_hbm.at[part], uv.at[part], u_sem.at[chunk]))

        def store(chunk):
            part = pl.ds(chunk * 2 * (span // ROWS_B), 2 * (span // ROWS_B))
            return pltpu.make_async_copy(ov.at[part], out_hbm.at[part], out_sem.at[chunk])

        for chunk in range(chunks):
            for load in loads(chunk):
                load.start()

        @pl.loop(0, chunks)
        def _(chunk):
            for load in loads(chunk):
                load.wait()
            scale, bias, weight = scale_ref[0], scale_ref[1], weight_ref[...]
            for tile in range(span):
                value = jnp.dot(weight, uv[chunk * span + tile], preferred_element_type=F32)
                hidden = hv[chunk * span + tile].astype(F32)
                for image in range(2):
                    half = slice(image * HALF, (image + 1) * HALF)
                    done = jnp.maximum(value[:, half] * scale + bias + hidden[:, half], 0.0)
                    ov[chunk * 2 * (span // ROWS_B) + 2 * (tile // ROWS_B) + image, tile % ROWS_B] = done.T.astype(BF16)
            store(chunk).start()

        @pl.loop(0, chunks)
        def _(chunk):
            store(chunk).wait()

    def forward(images, w_a, bn_a, w_down, bn_down, w_in, bn_in, w_mid, bn_mid, w_out, bn_out):
        images_count = images.shape[0]
        pairs = images_count // 2
        x = jnp.transpose(images, (0, 1, 3, 2))
        layers = w_a.shape[0] + 1 + 3 * w_in.shape[0]
        steps = 3 + w_in.shape[0]
        vmem = pl.BlockSpec(memory_space=pltpu.VMEM)
        hbm = pl.BlockSpec(memory_space=pl.ANY)
        dma = pltpu.SemaphoreType.DMA
        tiles = pairs * ROWS_B
        hidden, branch, scale, weight = pl.pallas_call(
            kernel,
            out_shape=(
                jax.ShapeDtypeStruct((tiles, HALF, LANES), BF16), jax.ShapeDtypeStruct((tiles, MID, LANES), BF16),
                jax.ShapeDtypeStruct((2, HALF, HALF), F32), jax.ShapeDtypeStruct((HALF, MID), BF16)),
            in_specs=[hbm] + [hbm, vmem] * 5,
            out_specs=(hbm, hbm, vmem, vmem),
            scratch_shapes=[
                pltpu.VMEM(w_a.shape, BF16), pltpu.VMEM(w_down.shape, BF16), pltpu.VMEM((w_in.shape[0], MID, HALF), BF16),
                pltpu.VMEM(w_mid.shape, BF16), pltpu.VMEM(w_out.shape, BF16), dma((5,)),
                pltpu.VMEM((LANES, LANES), BF16),
                pltpu.VMEM((w_a.shape[0], HALF, BAND_A), BF16),
                pltpu.VMEM((HALF, DOWN_K), BF16),
                pltpu.VMEM((w_in.shape[0], HALF, BAND_B), BF16),
                pltpu.VMEM((w_in.shape[0], HALF, MID), BF16),
                pltpu.VMEM((pairs, 2, ROWS_A, CIN, LANES), BF16),
                pltpu.VMEM((2, images_count, CIN, LANES), BF16),
                pltpu.VMEM((pairs, ROWS_A + 2, HALF, LANES), BF16),
                pltpu.VMEM((pairs, ROWS_B + 2, TRIPLE, LANES), BF16),
                pltpu.VMEM((pairs * ROWS_A, MID, LANES), F32),
                pltpu.VMEM((pairs * ROWS_B, HALF, LANES), F32),
                pltpu.VMEM((pairs * ROWS_B, HALF, LANES), BF16),
                pltpu.VMEM((pairs * ROWS_B, MID, LANES), BF16),
                pltpu.VMEM((2, HALF, HALF), F32),
                pltpu.VMEM((2, HALF, HALF), F32),
                pltpu.VMEM((layers, groups, PAIR_SUB, HALF), F32),
                dma((pairs,)), dma((pairs // UNROLL + 1,)), dma((steps, 2, pairs // UNROLL)), dma((steps, 2, pairs // UNROLL)),
                pltpu.VMEM((steps, 2, UNROLL, MID, LANES), F32), dma((steps, 2, UNROLL)), dma((steps, 2, UNROLL)),
                dma((layers, groups)), dma((layers, groups)),
            ],
            compiler_params=pltpu.CompilerParams(
                collective_id=0, has_side_effects=True, vmem_limit_bytes=67043328),
            name="conv_stack",
        )(x, w_a, bn_a, w_down, bn_down, jnp.transpose(w_in, (0, 2, 1)), bn_in, w_mid, bn_mid, w_out, bn_out)
        return pl.pallas_call(
            last_kernel,
            out_shape=jax.ShapeDtypeStruct((images_count, ROWS_B, HALF, HALF), BF16),
            in_specs=[hbm, hbm, vmem, vmem],
            out_specs=hbm,
            scratch_shapes=[
                pltpu.VMEM((tiles, HALF, LANES), BF16), pltpu.VMEM((tiles, MID, LANES), BF16),
                pltpu.VMEM((images_count, ROWS_B, HALF, HALF), BF16),
                dma((LAST_STEPS,)), dma((LAST_STEPS,)), dma((LAST_STEPS,))],
            name="last_layer",
        )(hidden, branch, scale, weight)

    act_spec = P("dp", "sp", None, None)
    return jax.shard_map(forward, mesh=mesh, in_specs=(act_spec,) + (P(),) * 10, out_specs=act_spec, check_vma=False)
```

```python
import functools

import jax
import jax.numpy as jnp
from jax import lax
from jax.experimental import pallas as pl
from jax.experimental.pallas import tpu as pltpu
from jax.sharding import PartitionSpec as P

NORM_EPS = 1e-5
MESH = pl.DeviceIdType.MESH
F32 = jnp.float32
BF16 = jnp.bfloat16
ROWS_A = 8
ROWS_B = 4
UNROLL = 4
LAST_STEPS = 4
LANES = 256
HALF = 128
MID = 64
CIN = 32
THREE = 96
TRIPLE = 192
DOWN_K = 384
BAND_A = 512
BAND_B = 768
FOUR = 4
SUB = 8
PAIR_SUB = 16


def solution(mesh):
    groups = mesh.shape["sp"]

    def kernel(x_hbm, raw_a_hbm, bn_a, raw_d_hbm, bn_d, wi_hbm, bn_i, raw_m_hbm, bn_m, raw_o_hbm, bn_o,
               h_hbm, u_hbm, scale_out, weight_out,
               raw_a, raw_d, wi, raw_m, raw_o, w_sem,
               perm, wa, wd, wm, wo, xv, xh, hs, us, za, zb, hb, ub, acc, ab, stat,
               x_sem, out_sem, halo_send, halo_recv, zh, early_send, early_recv, stat_send, stat_recv):
        pairs = xv.shape[0]
        me = lax.axis_index("sp")
        count_a = float(2 * pairs * ROWS_A * LANES * groups)
        count_b = float(2 * pairs * ROWS_B * HALF * groups)

        def sweep(body, *later, before=None, after=None, first=0):
            @pl.loop(first, pairs // UNROLL)
            def _(step):
                if before is not None:
                    before(step)
                for stage in (body,) + later:
                    sums = [stage(step * UNROLL + part) for part in range(UNROLL)]
                if after is not None:
                    after(step)
                if sums[0] is not None:
                    channels = sums[0].shape[1]
                    acc[:, 0:channels] += sum(sums[1:], sums[0])

        def x_copy(pair):
            return pltpu.make_async_copy(x_hbm.at[pl.ds(2 * pair, 2)], xv.at[pair], x_sem.at[pair])

        @sweep
        def _(pair):
            x_copy(pair).start()

        loads = [pltpu.make_async_copy(src, dst, w_sem.at[index]) for index, (src, dst) in enumerate(
            [(raw_a_hbm, raw_a), (raw_d_hbm, raw_d), (raw_m_hbm, raw_m), (raw_o_hbm, raw_o), (wi_hbm, wi)])]
        for load in loads:
            load.start()

        barrier = pltpu.get_barrier_semaphore()
        for hop in range(1, groups):
            pl.semaphore_signal(barrier, inc=1, device_id={"sp": lax.rem(me + hop, groups)}, device_id_type=MESH)
        pl.semaphore_wait(barrier, groups - 1)

        def halo_copy(step, side, chunk, refs, peer):
            src, dst = refs[side](chunk * UNROLL)
            return pltpu.make_async_remote_copy(
                src_ref=src, dst_ref=dst, send_sem=halo_send.at[step, side, chunk],
                recv_sem=halo_recv.at[step, side, chunk], device_id={"sp": peer}, device_id_type=MESH)

        def exchange(step, refs, chunk, sides=(0, 1)):
            for side in sides:
                @pl.when(me < groups - 1 if side == 0 else me > 0)
                def _():
                    halo_copy(step, side, chunk, refs, me + 1 if side == 0 else me - 1).start()

        def settle(step, refs, chunk, sides=(0, 1)):
            for side in sides:
                @pl.when(me > 0 if side == 0 else me < groups - 1)
                def _():
                    halo_copy(step, side, chunk, refs, me - 1 if side == 0 else me + 1).wait_recv()

                @pl.when(me < groups - 1 if side == 0 else me > 0)
                def _():
                    halo_copy(step, side, chunk, refs, me + 1 if side == 0 else me - 1).wait_send()

        def x_part(row, slot):
            return lambda pair: (x_hbm.at[pl.ds(2 * pair, 2 * UNROLL), row], xh.at[slot, pl.ds(2 * pair, 2 * UNROLL)])

        def h_part(row, slot):
            return lambda pair: (hs.at[pl.ds(pair, UNROLL), row, CIN:THREE], hs.at[pl.ds(pair, UNROLL), slot, CIN:THREE])

        def u_part(row, slot):
            return lambda pair: (us.at[pl.ds(pair, UNROLL), row, MID:HALF], us.at[pl.ds(pair, UNROLL), slot, MID:HALF])

        def early_copy(step, side, part, rows, peer):
            return pltpu.make_async_remote_copy(
                src_ref=za.at[part * rows + (rows - 1 if side == 0 else 0)], dst_ref=zh.at[step, side, part],
                send_sem=early_send.at[step, side, part], recv_sem=early_recv.at[step, side, part],
                device_id={"sp": peer}, device_id_type=MESH)

        def early(step, rows, sides=(0, 1)):
            for side in sides:
                @pl.when(me < groups - 1 if side == 0 else me > 0)
                def _():
                    for part in range(UNROLL):
                        early_copy(step, side, part, rows, me + 1 if side == 0 else me - 1).start()

        def settle_early(step, rows, put, sides=(0, 1)):
            for side in sides:
                @pl.when(me > 0 if side == 0 else me < groups - 1)
                def _():
                    for part in range(UNROLL):
                        early_copy(step, side, part, rows, me - 1 if side == 0 else me + 1).wait_recv()
                    for part in range(UNROLL):
                        put(part, 0 if side == 0 else rows + 1, norm_relu(zh[step, side, part]))

                @pl.when(me < groups - 1 if side == 0 else me > 0)
                def _():
                    for part in range(UNROLL):
                        early_copy(step, side, part, rows, me + 1 if side == 0 else me - 1).wait_send()

        def first_chunk(*stages):
            for stage in stages:
                sums = [stage(part) for part in range(UNROLL)]
            if sums[0] is not None:
                acc[:, 0:sums[0].shape[1]] += sum(sums[1:], sums[0])

        x_refs = (x_part(ROWS_A - 1, 0), x_part(0, 1))
        h_refs = (h_part(ROWS_A, 0), h_part(1, ROWS_A + 1))
        u_refs = (u_part(ROWS_B, 0), u_part(1, ROWS_B + 1))

        @pl.loop(0, pairs // UNROLL)
        def _(chunk):
            exchange(0, x_refs, chunk)

        @pl.when(me == 0)
        def _():
            xh[0] = jnp.zeros(xh.shape[1:], BF16)

            @sweep
            def _(pair):
                hs[pair, 0] = jnp.zeros(hs.shape[2:], BF16)
                us[pair, 0] = jnp.zeros(us.shape[2:], BF16)

        @pl.when(me == groups - 1)
        def _():
            xh[1] = jnp.zeros(xh.shape[1:], BF16)

            @sweep
            def _(pair):
                hs[pair, ROWS_A + 1] = jnp.zeros(hs.shape[2:], BF16)
                us[pair, ROWS_B + 1] = jnp.zeros(us.shape[2:], BF16)

        def turn(block):
            return block.astype(F32).T.astype(BF16)

        def prepare_a(layer):
            for row in range(FOUR):
                lines = []
                for plane in range(FOUR):
                    tiles = []
                    for out_row in range(2):
                        for phase in range(2):
                            high, wide = row - out_row, plane - phase
                            inside = 0 <= high < 3 and 0 <= wide < 3
                            tiles.append(raw_a[layer, high, wide].astype(F32) if inside else jnp.zeros((CIN, CIN), F32))
                    lines.append(jnp.concatenate(tiles, axis=1))
                wa[layer, :, HALF * row:HALF * row + HALF] = turn(jnp.concatenate(lines, axis=0))

        def prepare_down():
            for high in range(3):
                lines = [jnp.zeros((CIN, HALF), BF16)] + [raw_d[high, wide] for wide in range(3)]
                wd[:, HALF * high:HALF * high + HALF] = turn(jnp.concatenate(lines, axis=0))

        def prepare_mid(block, parts):
            for part in parts:
                lines = []
                for line in (2 * part, 2 * part + 1):
                    row, wide = divmod(line, 3)
                    tiles = []
                    for out_row in range(2):
                        high = row - out_row
                        inside = 0 <= high < 3
                        tiles.append(raw_m[block, high, wide].astype(F32) if inside else jnp.zeros((MID, MID), F32))
                    lines.append(jnp.concatenate(tiles, axis=1))
                wm[block, :, HALF * part:HALF * part + HALF] = turn(jnp.concatenate(lines, axis=0))

        def prepare_out(block):
            wo[block] = turn(raw_o[block])

        def shift(value, step):
            lane = lax.broadcasted_iota(jnp.int32, (value.shape[0], HALF), 1)
            edge = 0 if step == 1 else 127
            halves = []
            for half in range(2):
                moved = pltpu.roll(value[:, half * HALF:(half + 1) * HALF], step % HALF, 1)
                halves.append(jnp.where(lane == edge, 0.0, moved))
            return jnp.concatenate(halves, axis=1)

        def put_planes(pair, row, even, odd, centre=True):
            hs[pair, row, 0:CIN] = shift(odd, 1).astype(BF16)
            if centre:
                hs[pair, row, CIN:MID] = even.astype(BF16)
                hs[pair, row, MID:THREE] = odd.astype(BF16)
            hs[pair, row, THREE:HALF] = shift(even, -1).astype(BF16)

        def put_mid(pair, row, value, centre=True):
            us[pair, row, 0:MID] = shift(value, 1).astype(BF16)
            if centre:
                us[pair, row, MID:HALF] = value.astype(BF16)
            us[pair, row, HALF:TRIPLE] = shift(value, -1).astype(BF16)

        def rebuild_a(pair, row):
            both = hs[pair, row, CIN:THREE].astype(F32)
            put_planes(pair, row, both[0:CIN], both[CIN:MID], centre=False)

        def rebuild_mid(pair, row):
            put_mid(pair, row, us[pair, row, MID:HALF].astype(F32), centre=False)

        def clear():
            acc[...] = jnp.zeros(acc.shape, F32)

        def tally(channels, *values):
            total, square = 0.0, 0.0
            for value in values:
                for half in range(2):
                    for row in range(0, value.shape[0], channels):
                        piece = value[row:row + channels, half * HALF:(half + 1) * HALF]
                        total, square = total + piece, square + piece * piece
            return jnp.stack([total, square])

        def moments(layer, params, count, during=None, early=None):
            channels = params.shape[1]
            for part in range(2):
                turned = jnp.concatenate([acc[part, 0:channels]] * (HALF // channels), axis=0).T.reshape(PAIR_SUB, SUB, HALF)
                stat[layer, me, SUB * part:SUB * part + SUB] = jnp.sum(turned, axis=0)
            copies = []
            for hop in range(1, groups):
                copies.append(pltpu.make_async_remote_copy(
                    src_ref=stat.at[layer, me], dst_ref=stat.at[layer, me],
                    send_sem=stat_send.at[layer, hop], recv_sem=stat_recv.at[layer, hop],
                    device_id={"sp": lax.rem(me + hop, groups)}, device_id_type=MESH))
            for copy in copies:
                copy.start()
            if early is not None:
                early()
            clear()
            if during is not None:
                during()
            for hop in range(1, groups):
                origin = lax.rem(me + groups - hop, groups)
                pltpu.make_async_remote_copy(
                    src_ref=stat.at[layer, origin], dst_ref=stat.at[layer, origin],
                    send_sem=stat_send.at[layer, hop], recv_sem=stat_recv.at[layer, hop],
                    device_id={"sp": origin}, device_id_type=MESH).wait_recv()
            for copy in copies:
                copy.wait_send()
            total = stat[layer, 0]
            for origin in range(1, groups):
                total = total + stat[layer, origin]

            def fold(block):
                return jnp.sum(block, axis=0, keepdims=True) / count

            mean, square = fold(total[0:SUB]), fold(total[SUB:PAIR_SUB])
            var = square - mean * mean
            wide = jnp.concatenate([params] * (HALF // channels), axis=1)
            scale = wide[0:1] * lax.rsqrt(var + NORM_EPS)
            bias = wide[1:2] - mean * scale
            ab[0] = jnp.broadcast_to(scale, (HALF, HALF)).T
            ab[1] = jnp.broadcast_to(bias, (HALF, HALF)).T

        def affine(value):
            rows = value.shape[0]
            scale, bias = ab[0, 0:rows], ab[1, 0:rows]
            return jnp.concatenate(
                [value[:, :HALF] * scale + bias, value[:, HALF:] * scale + bias], axis=1)

        def norm_relu(value):
            return jnp.maximum(affine(value), 0.0)

        def mm(left, right):
            return jnp.dot(left, right, preferred_element_type=F32)

        clear()
        loads[0].wait()
        prepare_a(0)

        lane_in = lax.broadcasted_iota(jnp.int32, (LANES, LANES), 0)
        lane_out = lax.broadcasted_iota(jnp.int32, (LANES, LANES), 1)
        source = jnp.where(lane_out < HALF, 2 * lane_out, 2 * lane_out - (LANES - 1))
        perm[...] = jnp.where(lane_in == source, 1.0, 0.0).astype(BF16)

        def split_rows(first, second, pair, row):
            put_planes(pair, row, jnp.concatenate([first[:, :HALF], second[:, :HALF]], axis=1),
                       jnp.concatenate([first[:, HALF:], second[:, HALF:]], axis=1))

        def conv_a(layer, pair, row, rows):
            window = hs[pair, row:row + rows + 2].reshape((rows + 2) * HALF, LANES)
            value = mm(wa[layer, 0:MID * rows, 0:HALF * (rows + 2)], window)
            za[pl.ds(pair * ROWS_A + row, rows)] = value.reshape(rows, MID, LANES)
            return value

        def norm_a(pair, row):
            value = norm_relu(za[pair * ROWS_A + row])
            put_planes(pair, row + 1, value[0:CIN], value[CIN:MID])

        def planes(pair):
            x_copy(pair).wait()
            for start in range(0, ROWS_A, FOUR):
                both = mm(xv[pair, :, start:start + FOUR].reshape(2 * FOUR * CIN, LANES), perm[...])
                both = both.reshape(2, FOUR, CIN, LANES)
                for row in range(FOUR):
                    split_rows(both[0, row], both[1, row], pair, start + row + 1)

        def inner_a(layer):
            return lambda pair: tally(CIN, *[conv_a(layer, pair, row, 2) for row in range(1, ROWS_A - 1, 2)])

        def outer_a(layer):
            return lambda pair: tally(CIN, conv_a(layer, pair, 0, 1), conv_a(layer, pair, ROWS_A - 1, 1))

        sweep(planes, inner_a(0))

        def halo_planes(pair):
            both = mm(xh[:, pl.ds(2 * pair, 2)].reshape(FOUR * CIN, LANES), perm[...]).reshape(2, 2, CIN, LANES)
            split_rows(both[0, 0], both[0, 1], pair, 0)
            split_rows(both[1, 0], both[1, 1], pair, ROWS_A + 1)

        sweep(halo_planes, outer_a(0), before=lambda chunk: settle(0, x_refs, chunk))

        def second_weights():
            for load in loads[1:]:
                load.wait()
            prepare_a(1)
            prepare_mid(0, (0, 1))

        def down_weights():
            prepare_down()
            prepare_mid(0, (2, 3))

        moments(0, bn_a[0], count_a, second_weights, lambda: early(1, ROWS_A))

        def norm_edges(pair):
            norm_a(pair, 0)
            norm_a(pair, ROWS_A - 1)

        def put_edge(pair, slot, value):
            put_planes(pair, slot, value[0:CIN], value[CIN:MID])

        sweep(norm_edges, after=lambda chunk: exchange(1, h_refs, chunk), first=1)
        first_chunk(norm_edges)

        def norm_inner(pair):
            for row in range(1, ROWS_A - 1):
                norm_a(pair, row)

        sweep(norm_inner, inner_a(1))

        def rebuild_both(pair):
            rebuild_a(pair, 0)
            rebuild_a(pair, ROWS_A + 1)

        settle_early(1, ROWS_A, put_edge)
        first_chunk(outer_a(1))
        sweep(rebuild_both, outer_a(1), before=lambda chunk: settle(1, h_refs, chunk), first=1)

        moments(1, bn_a[1], count_a, down_weights, lambda: early(2, ROWS_A, (1,)))

        def conv_down(pair, row):
            window = hs[pair, 2 * row + 1:2 * row + FOUR].reshape(DOWN_K, LANES)
            value = mm(wd[...], window)
            zb[pair * ROWS_B + row] = value
            return value

        sweep(lambda pair: norm_a(pair, 0), after=lambda chunk: exchange(2, h_refs, chunk, (1,)), first=1)
        first_chunk(lambda pair: norm_a(pair, 0))

        def norm_below(pair):
            for row in range(1, ROWS_A):
                norm_a(pair, row)

        sweep(norm_below, lambda pair: tally(HALF, *[conv_down(pair, row) for row in range(ROWS_B - 1)]))

        def down_edge(pair):
            return tally(HALF, conv_down(pair, ROWS_B - 1))

        settle_early(2, ROWS_A, put_edge, (1,))
        first_chunk(down_edge)
        sweep(lambda pair: rebuild_a(pair, ROWS_A + 1), down_edge,
              before=lambda chunk: settle(2, h_refs, chunk, (1,)), first=1)

        moments(2, bn_d[...], count_b, lambda: prepare_mid(0, (FOUR, 5)))

        def conv_in(block, index):
            value = mm(wi[block], hb[index])
            za[index] = value
            return value

        def conv_mid(block, pair, row, rows):
            window = us[pair, row:row + rows + 2].reshape((rows + 2) * TRIPLE, LANES)
            value = mm(wm[block, 0:MID * rows, 0:TRIPLE * (rows + 2)], window)
            za[pl.ds(pair * ROWS_B + row, rows)] = value.reshape(rows, MID, LANES)
            return value

        def norm_mid(pair, row):
            put_mid(pair, row + 1, norm_relu(za[pair * ROWS_B + row]))

        def all_in(block):
            return lambda pair: tally(MID, *[conv_in(block, pair * ROWS_B + row) for row in range(ROWS_B)])

        def first_hidden(pair):
            for row in range(ROWS_B):
                index = pair * ROWS_B + row
                hb[index] = norm_relu(zb[index]).astype(BF16)

        sweep(first_hidden, all_in(0))

        blocks = wi.shape[0]
        for block in range(blocks):
            layer, step = 3 + 3 * block, 3 + block
            moments(layer, bn_i[block], count_b, lambda: prepare_out(block),
                    lambda: early(step, ROWS_B))

            def mid_edges(pair):
                norm_mid(pair, 0)
                norm_mid(pair, ROWS_B - 1)

            def mid_conv(pair):
                return tally(MID, conv_mid(block, pair, 0, 1), conv_mid(block, pair, ROWS_B - 1, 1))

            sweep(mid_edges, after=lambda chunk: exchange(step, u_refs, chunk), first=1)
            first_chunk(mid_edges)

            def mid_inner(pair):
                for row in range(1, ROWS_B - 1):
                    norm_mid(pair, row)

            def mid_outer(pair):
                rebuild_mid(pair, 0)
                rebuild_mid(pair, ROWS_B + 1)

            sweep(mid_inner, lambda pair: tally(MID, conv_mid(block, pair, 1, 2)))
            settle_early(step, ROWS_B, put_mid)
            first_chunk(mid_conv)
            sweep(mid_outer, mid_conv, before=lambda chunk: settle(step, u_refs, chunk), first=1)

            last = block == blocks - 1
            moments(layer + 1, bn_m[block], count_b, None if last else lambda: prepare_mid(block + 1, (0, 1, 2)))

            if last:
                h_copy = pltpu.make_async_copy(hb, h_hbm, out_sem.at[pairs // UNROLL])
                h_copy.start()
                weight_out[...] = wo[block]

            def u_copy(chunk):
                span = pl.ds(chunk * UNROLL * ROWS_B, UNROLL * ROWS_B)
                return pltpu.make_async_copy(ub.at[span], u_hbm.at[span], out_sem.at[chunk])

            def all_out(pair):
                values = []
                for row in range(ROWS_B):
                    index = pair * ROWS_B + row
                    hidden = norm_relu(za[index]).astype(BF16)
                    values.append(mm(wo[block], hidden))
                    if last:
                        ub[index] = hidden
                    else:
                        zb[index] = values[-1]
                return tally(HALF, *values)

            sweep(all_out, after=(lambda chunk: u_copy(chunk).start()) if last else None)
            moments(layer + 2, bn_o[block], count_b, None if last else lambda: prepare_mid(block + 1, (3, FOUR, 5)))

            if not last:
                def next_hidden(pair):
                    for row in range(ROWS_B):
                        index = pair * ROWS_B + row
                        hb[index] = jnp.maximum(affine(zb[index]) + hb[index].astype(F32), 0.0).astype(BF16)

                sweep(next_hidden, all_in(block + 1))
            else:
                scale_out[...] = ab[...]
                h_copy.wait()

                @pl.loop(0, pairs // UNROLL)
                def _(chunk):
                    u_copy(chunk).wait()

    def last_kernel(h_hbm, u_hbm, scale_ref, weight_ref, out_hbm, hv, uv, ov, h_sem, u_sem, out_sem):
        chunks = h_sem.shape[0]
        span = hv.shape[0] // chunks

        def loads(chunk):
            part = pl.ds(chunk * span, span)
            return (pltpu.make_async_copy(h_hbm.at[part], hv.at[part], h_sem.at[chunk]),
                    pltpu.make_async_copy(u_hbm.at[part], uv.at[part], u_sem.at[chunk]))

        def store(chunk):
            part = pl.ds(chunk * 2 * (span // ROWS_B), 2 * (span // ROWS_B))
            return pltpu.make_async_copy(ov.at[part], out_hbm.at[part], out_sem.at[chunk])

        for chunk in range(chunks):
            for load in loads(chunk):
                load.start()

        @pl.loop(0, chunks)
        def _(chunk):
            for load in loads(chunk):
                load.wait()
            scale, bias, weight = scale_ref[0], scale_ref[1], weight_ref[...]
            for tile in range(span):
                value = jnp.dot(weight, uv[chunk * span + tile], preferred_element_type=F32)
                hidden = hv[chunk * span + tile].astype(F32)
                for image in range(2):
                    half = slice(image * HALF, (image + 1) * HALF)
                    done = jnp.maximum(value[:, half] * scale + bias + hidden[:, half], 0.0)
                    ov[chunk * 2 * (span // ROWS_B) + 2 * (tile // ROWS_B) + image, tile % ROWS_B] = done.T.astype(BF16)
            store(chunk).start()

        @pl.loop(0, chunks)
        def _(chunk):
            store(chunk).wait()

    def forward(images, w_a, bn_a, w_down, bn_down, w_in, bn_in, w_mid, bn_mid, w_out, bn_out):
        images_count = images.shape[0]
        pairs = images_count // 2
        x = jnp.transpose(images, (0, 1, 3, 2))
        layers = w_a.shape[0] + 1 + 3 * w_in.shape[0]
        steps = 3 + w_in.shape[0]
        vmem = pl.BlockSpec(memory_space=pltpu.VMEM)
        hbm = pl.BlockSpec(memory_space=pl.ANY)
        dma = pltpu.SemaphoreType.DMA
        tiles = pairs * ROWS_B
        hidden, branch, scale, weight = pl.pallas_call(
            kernel,
            out_shape=(
                jax.ShapeDtypeStruct((tiles, HALF, LANES), BF16), jax.ShapeDtypeStruct((tiles, MID, LANES), BF16),
                jax.ShapeDtypeStruct((2, HALF, HALF), F32), jax.ShapeDtypeStruct((HALF, MID), BF16)),
            in_specs=[hbm] + [hbm, vmem] * 5,
            out_specs=(hbm, hbm, vmem, vmem),
            scratch_shapes=[
                pltpu.VMEM(w_a.shape, BF16), pltpu.VMEM(w_down.shape, BF16), pltpu.VMEM((w_in.shape[0], MID, HALF), BF16),
                pltpu.VMEM(w_mid.shape, BF16), pltpu.VMEM(w_out.shape, BF16), dma((5,)),
                pltpu.VMEM((LANES, LANES), BF16),
                pltpu.VMEM((w_a.shape[0], HALF, BAND_A), BF16),
                pltpu.VMEM((HALF, DOWN_K), BF16),
                pltpu.VMEM((w_in.shape[0], HALF, BAND_B), BF16),
                pltpu.VMEM((w_in.shape[0], HALF, MID), BF16),
                pltpu.VMEM((pairs, 2, ROWS_A, CIN, LANES), BF16),
                pltpu.VMEM((2, images_count, CIN, LANES), BF16),
                pltpu.VMEM((pairs, ROWS_A + 2, HALF, LANES), BF16),
                pltpu.VMEM((pairs, ROWS_B + 2, TRIPLE, LANES), BF16),
                pltpu.VMEM((pairs * ROWS_A, MID, LANES), F32),
                pltpu.VMEM((pairs * ROWS_B, HALF, LANES), F32),
                pltpu.VMEM((pairs * ROWS_B, HALF, LANES), BF16),
                pltpu.VMEM((pairs * ROWS_B, MID, LANES), BF16),
                pltpu.VMEM((2, HALF, HALF), F32),
                pltpu.VMEM((2, HALF, HALF), F32),
                pltpu.VMEM((layers, groups, PAIR_SUB, HALF), F32),
                dma((pairs,)), dma((pairs // UNROLL + 1,)), dma((steps, 2, pairs // UNROLL)), dma((steps, 2, pairs // UNROLL)),
                pltpu.VMEM((steps, 2, UNROLL, MID, LANES), F32), dma((steps, 2, UNROLL)), dma((steps, 2, UNROLL)),
                dma((layers, groups)), dma((layers, groups)),
            ],
            compiler_params=pltpu.CompilerParams(
                collective_id=0, has_side_effects=True, vmem_limit_bytes=67043328),
            name="conv_stack",
        )(x, w_a, bn_a, w_down, bn_down, jnp.transpose(w_in, (0, 2, 1)), bn_in, w_mid, bn_mid, w_out, bn_out)
        return pl.pallas_call(
            last_kernel,
            out_shape=jax.ShapeDtypeStruct((images_count, ROWS_B, HALF, HALF), BF16),
            in_specs=[hbm, hbm, vmem, vmem],
            out_specs=hbm,
            scratch_shapes=[
                pltpu.VMEM((tiles, HALF, LANES), BF16), pltpu.VMEM((tiles, MID, LANES), BF16),
                pltpu.VMEM((images_count, ROWS_B, HALF, HALF), BF16),
                dma((LAST_STEPS,)), dma((LAST_STEPS,)), dma((LAST_STEPS,))],
            name="last_layer",
        )(hidden, branch, scale, weight)

    act_spec = P("dp", "sp", None, None)
    return jax.shard_map(forward, mesh=mesh, in_specs=(act_spec,) + (P(),) * 10, out_specs=act_spec, check_vma=False)
```
